256 devices in a mesh: rep: 2 (over core), dp: 128 (over x, y, z).
Axes of the slice: x: 4, y: 4, z: 8, core: 2. Of those that a mesh axis runs over, the one named last changes fastest.
Arguments:
- x: bfloat16 [256, 1024, 512], P(('rep', 'dp')), parts along dimension 0
- dy: bfloat16 [256, 1024, 512], P(('rep', 'dp')), parts along dimension 0
- w_gate: bfloat16 [2, 512, 8192], replicated
- w_up: bfloat16 [2, 512, 8192], replicated
- w_down: bfloat16 [2, 8192, 512], replicated
- m_w_gate: float32 [2, 512, 8192], P(None, 'dp')
- m_w_up: float32 [2, 512, 8192], P(None, 'dp')
- m_w_down: float32 [2, 8192, 512], P(None, 'dp')
- v_w_gate: float32 [2, 512, 8192], P(None, 'dp')
- v_w_up: float32 [2, 512, 8192], P(None, 'dp')
- v_w_down: float32 [2, 8192, 512], P(None, 'dp')
Outputs:
- output 1: bfloat16 [4, 512, 8192], P('rep'), parts along dimension 0
- output 2: bfloat16 [4, 512, 8192], P('rep'), parts along dimension 0
- output 3: bfloat16 [4, 8192, 512], P('rep'), parts along dimension 0
- output 4: float32 [4, 512, 8192], P('rep', 'dp'), parts along dimension 0
- output 5: float32 [4, 512, 8192], P('rep', 'dp'), parts along dimension 0
- output 6: float32 [4, 8192, 512], P('rep', 'dp'), parts along dimension 0
- output 7: float32 [4, 512, 8192], P('rep', 'dp'), parts along dimension 0
- output 8: float32 [4, 512, 8192], P('rep', 'dp'), parts along dimension 0
- output 9: float32 [4, 8192, 512], P('rep', 'dp'), parts along dimension 0
There are 2 independent parts. The reference program is written for one: setup_inputs(seed, part) draws one part's arguments, and reference() takes and returns one part's arrays. A program takes and returns all parts, laid end to end along the dimension named above; an argument that names none is the same for every part.
All inputs are finite; a program needn't handle non-finite values.
Results may differ from the reference program's by a relative error of at most 0.022.
Values are sent between devices in bfloat16 or wider.
A program may use at most 768 MiB of HBM per device.

```python
import jax
import jax.numpy as jnp
from jax import lax

SEQUENCES = 128
TOKENS = 1024
D = 512
FF = 8192
LAYERS = 2
NAMES = ("w_gate", "w_up", "w_down")
SHAPES = {"w_gate": (LAYERS, D, FF), "w_up": (LAYERS, D, FF), "w_down": (LAYERS, FF, D)}


def bump(key, n, height):
    away = (jnp.arange(n, dtype=jnp.int32) - jax.random.randint(key, (), 0, n, jnp.int32)) % n
    return jnp.where(away < n // 8, height, 1.0)


def together(key, own, strength):
    shared = jax.random.normal(key, own.shape[1:], jnp.float32)
    return (own + strength * shared) * lax.rsqrt(1 + strength * strength)


def setup_inputs(seed: int = 0, part: int = 0) -> dict:
    kx, kdy, ka, kb, kz, kf, kh, kl, *keys = jax.random.split(jax.random.key(seed), 8 + 3 * len(NAMES))
    kx, kdy, ka, kb = (jax.random.fold_in(k, part) for k in (kx, kdy, ka, kb))
    kw, km, kv = (keys[i::3] for i in range(3))
    shape = (SEQUENCES, TOKENS, D)
    much_x, much_dy = jax.random.uniform(kz, (2,), jnp.float32, 0.0, 1.0)
    loud = 2.0 ** jax.random.uniform(jax.random.fold_in(kz, 1), (), jnp.float32, -1.0, 2.0)
    layers = 2.0 ** jax.random.uniform(kl, (LAYERS, 1, 1), jnp.float32, -1.0, 1.0)
    x = together(ka, jax.random.normal(kx, shape, jnp.float32), much_x) * bump(kf, D, 4.0)
    dy = together(kb, jax.random.normal(kdy, shape, jnp.float32), much_dy)
    drawn = {"x": x.astype(jnp.bfloat16), "dy": (loud * dy * (SEQUENCES * TOKENS) ** -0.5).astype(jnp.bfloat16)}
    for key, name in zip(kw, NAMES, strict=True):
        w = jax.random.normal(key, SHAPES[name], jnp.float32) * SHAPES[name][1] ** -0.5
        drawn[name] = (w * {"w_gate": 1.0, "w_up": bump(kh, FF, 4.0), "w_down": layers}[name]).astype(jnp.bfloat16)
    for key, name in zip(km, NAMES, strict=True):
        drawn[f"m_{name}"] = 0.1 * jax.random.normal(key, SHAPES[name], jnp.float32)
    for key, name in zip(kv, NAMES, strict=True):
        drawn[f"v_{name}"] = loud * loud * jax.random.uniform(key, SHAPES[name], jnp.float32, 0.05, 0.15)
    return drawn


def matmul(a, w):
    return jnp.dot(a, w, preferred_element_type=jnp.float32).astype(jnp.bfloat16)


def normed(h):
    wide = h.astype(jnp.float32)
    scale = lax.rsqrt(jnp.mean(wide**2, -1, keepdims=True) + 1e-6)
    return (wide * scale).astype(jnp.bfloat16)


def layer(h, w):
    a = normed(h)
    gate = jnp.dot(a, w["w_gate"], preferred_element_type=jnp.float32)
    up = jnp.dot(a, w["w_up"], preferred_element_type=jnp.float32)
    return h + matmul((jax.nn.silu(gate) * up).astype(jnp.bfloat16), w["w_down"])


def adamw(w, m, v, g):
    m = 0.9 * m + 0.1 * g
    v = 0.95 * v + 0.05 * g * g
    step = m * lax.rsqrt(v + 1e-8) + 0.1 * w
    return (w - 0.02 * step).astype(jnp.bfloat16), m, v


def stack(weights, h):
    return lax.scan(lambda h, w: (layer(h, w), None), h, weights)[0]


def reference(x, dy, w_gate, w_up, w_down, m_w_gate, m_w_up, m_w_down, v_w_gate, v_w_up, v_w_down):
    weights = dict(zip(NAMES, (w_gate, w_up, w_down), strict=True))

    def take(so_far, sequence):
        h, by_y = sequence
        _, back = jax.vjp(lambda w: stack(w, h), weights)
        return jax.tree.map(lambda total, term: total + term.astype(jnp.float32), so_far, back(by_y)[0]), None

    none_yet = {name: jnp.zeros(w.shape, jnp.float32) for name, w in weights.items()}
    by_weights, _ = lax.scan(take, none_yet, (x, dy))
    gradients = [by_weights[name].astype(jnp.bfloat16).astype(jnp.float32) for name in NAMES]
    new = [
        adamw(w.astype(jnp.float32), m, v, g)
        for w, m, v, g in zip((w_gate, w_up, w_down), (m_w_gate, m_w_up, m_w_down), (v_w_gate, v_w_up, v_w_down), gradients, strict=True)
    ]
    return tuple(one[which] for which in range(3) for one in new)
```

```python
import functools

import jax
import jax.numpy as jnp
from jax import lax
from jax.experimental import pallas as pl
from jax.experimental.pallas import tpu as pltpu
from jax.sharding import PartitionSpec as P

GRID = (4, 4, 8)
BF, F32 = jnp.bfloat16, jnp.float32
MESH = pl.DeviceIdType.MESH
VMEM_LIMIT = 66_000_000
LAG = 2
SLOTS = 6
JOBS = 4


def dot(a, b, dims=((1,), (0,))):
    return lax.dot_general(a, b, (dims, ((), ())), preferred_element_type=F32)


def normed(h):
    wide = h.astype(F32)
    scale = lax.rsqrt(jnp.mean(wide**2, -1, keepdims=True) + 1e-6)
    return (wide * scale).astype(BF)


def place():
    nx, ny, nz = GRID
    me = lax.axis_index("dp")
    at = (lax.div(me, ny * nz), lax.rem(lax.div(me, nz), ny), lax.rem(me, nz))

    def neighbour(axis, step):
        c = list(at)
        c[axis] = lax.rem(at[axis] + (step + GRID[axis]), GRID[axis])
        return (c[0] * ny + c[1]) * nz + c[2]

    return at, neighbour


def meet(neighbour):
    barrier = pltpu.get_barrier_semaphore()
    for axis in range(3):
        for step in (1, -1):
            pl.semaphore_signal(barrier, inc=1, device_id={"dp": neighbour(axis, step)}, device_id_type=MESH)
    pl.semaphore_wait(barrier, 6)


class Sender:
    def __init__(self, axis, at, neighbour, send, recv):
        self.n, self.p = GRID[axis], at[axis]
        self.to = (neighbour(axis, 1), neighbour(axis, -1))
        self.send, self.recv = send, recv

    def block(self, step):
        return lax.rem(self.p + (step + self.n), self.n)

    def copy(self, step, slot, d, src, dst):
        return pltpu.make_async_remote_copy(
            src_ref=src, dst_ref=dst, send_sem=self.send.at[step, slot, d], recv_sem=self.recv.at[step, slot, d],
            device_id={"dp": self.to[d]}, device_id_type=MESH,
        )

    def wait(self, step, slot, refs):
        for d in (0, 1):
            c = self.copy(step, slot, d, refs[d], refs[d])
            c.wait_recv()
            c.wait_send()


def forward_kernel(x_ref, wg, wu, wd, a_all, at_all, h1, acc):
    i = pl.program_id(0)

    @pl.when(i == 0)
    def _():
        a = normed(x_ref[...])
        a_all[0] = a
        at_all[0] = a.T
        acc[...] = jnp.zeros_like(acc)

    a = a_all[0]
    gate = dot(a, wg[0])
    up = dot(a, wu[0])
    hidden = (gate * jax.nn.sigmoid(gate) * up).astype(BF)
    acc[...] += dot(hidden, wd[0])

    @pl.when(i == pl.num_programs(0) - 1)
    def _():
        h = x_ref[...] + acc[...].astype(BF)
        h1[...] = h
        a = normed(h)
        a_all[1] = a
        at_all[1] = a.T


def forward(x, wg, wu, wd):
    (tokens, d), ff = x.shape, wg.shape[2]
    f = ff // 16
    return pl.pallas_call(
        forward_kernel,
        grid=(16,),
        in_specs=[
            pl.BlockSpec(memory_space=pltpu.VMEM),
            pl.BlockSpec((1, d, f), lambda i: (0, 0, i)),
            pl.BlockSpec((1, d, f), lambda i: (0, 0, i)),
            pl.BlockSpec((1, f, d), lambda i: (0, i, 0)),
        ],
        out_specs=[pl.BlockSpec(memory_space=pltpu.VMEM)] * 3,
        out_shape=[
            jax.ShapeDtypeStruct((2, tokens, d), BF),
            jax.ShapeDtypeStruct((2, d, tokens), BF),
            jax.ShapeDtypeStruct((tokens, d), BF),
        ],
        scratch_shapes=[pltpu.VMEM((tokens, d), F32)],
        compiler_params=pltpu.CompilerParams(vmem_limit_bytes=VMEM_LIMIT, dimension_semantics=("arbitrary",)),
        name="forward",
    )(x, wg, wu, wd)


def compute(layer, blocks, a_all, at_all, dh, wg, wu, wd, hid, dgate, dup, da):
    tokens = dgate.shape[0]
    rows = tokens // blocks
    for b in range(blocks):
        s = pl.ds(b * rows, rows)
        a = a_all[layer, s]
        gate = dot(a, wg[0])
        up = dot(a, wu[0])
        ct = dot(dh[layer, s], wd[0], ((1,), (1,))).astype(BF).astype(F32)
        sig = jax.nn.sigmoid(gate)
        silu = gate * sig
        hid[s] = (silu * up).astype(BF)
        dup[s] = (ct * silu).astype(BF)
        dgate[s] = (ct * up * (sig + silu * (1.0 - sig))).astype(BF)

    @pl.when(layer == 1)
    def _():
        da[...] += dot(dgate[...], wg[0], ((1,), (1,))) + dot(dup[...], wu[0], ((1,), (1,)))

    at = at_all[layer]
    return dot(at, dgate[...]), dot(at, dup[...]), dot(hid[...], dh[layer], ((0,), (0,)))


def reduce_kernel(a_all, at_all, dy, h1, wg, wu, wd, out_g, out_u, out_d, *scratch):
    (hid, dgate, dup, da, dh,
     own_g, own_u, own_d, acc_g2, acc_u2, acc_g3, acc_u3, acc_d2, acc_d3,
     rg, ru, rd, sg, su, sd, sems) = scratch
    nx, ny, nz = GRID
    chunks = nx * ny
    total = 2 * chunks
    f = wg.shape[2]
    t = pl.program_id(0)
    at, neighbour = place()
    x_, y_, z_ = at

    senders = {
        name: Sender(axis, at, neighbour, *sem)
        for (name, axis), sem in zip(
            (("g1", 0), ("g2", 1), ("g3", 2), ("u1", 1), ("u2", 0), ("u3", 2), ("d1", 2), ("d2", 1), ("d3", 0)), sems, strict=True
        )
    }

    def halves(array, ref):
        if array in ("g1", "g2", "d1", "d2", "d3"):
            h = ref.shape[-2] // 2
            return ref.at[pl.ds(0, h)], ref.at[pl.ds(h, h)]
        if array == "u1":
            return ref.at[pl.ds(0, nx // 2)], ref.at[pl.ds(nx // 2, nx // 2)]
        if array == "u2":
            h = ref.shape[-2] // 2
            return ref.at[pl.ds(0, h)], ref.at[pl.ds(h, h)]
        h = ref.shape[-1] // 2
        return ref.at[:, pl.ds(0, h)], ref.at[:, pl.ds(h, h)]

    def first(array, slot, own, recv):
        s = senders[array]

        def start():
            for d, half in enumerate(halves(array, own(s.block(s.n // 2)))):
                s.copy(0, slot, d, half, recv[0].at[slot, d]).start()

        def middle(j):
            s.wait(j - 1, slot, [recv[j - 1].at[slot, d] for d in (0, 1)])
            q = s.n // 2 - j
            for d in (0, 1):
                block = own(s.block(q if d == 0 else -q))
                into = halves(array, block)[d] if j == 1 else block
                into[...] = (into[...].astype(F32) + recv[j - 1][slot, d].astype(F32)).astype(BF)
                s.copy(j, slot, d, block, recv[j].at[slot, d]).start()

        def last():
            j = s.n // 2
            s.wait(j - 1, slot, [recv[j - 1].at[slot, d] for d in (0, 1)])
            return own(s.p)[...].astype(F32) + recv[j - 1][slot, 0].astype(F32) + recv[j - 1][slot, 1].astype(F32)

        return start, middle, last

    def later(array, slot, own, recv, stage):
        s = senders[array]

        def start():
            for d, half in enumerate(halves(array, own(s.block(s.n // 2)))):
                stage[0][slot, d] = half[...].astype(BF)
                s.copy(0, slot, d, stage[0].at[slot, d], recv[0].at[slot, d]).start()

        def middle(j):
            s.wait(j - 1, slot, [recv[j - 1].at[slot, d] for d in (0, 1)])
            q = s.n // 2 - j
            for d in (0, 1):
                block = own(s.block(q if d == 0 else -q))
                into = halves(array, block)[d] if j == 1 else block
                into[...] = into[...] + recv[j - 1][slot, d].astype(F32)
                stage[j][slot, d] = block[...].astype(BF)
                s.copy(j, slot, d, stage[j].at[slot, d], recv[j].at[slot, d]).start()

        def last():
            j = s.n // 2
            s.wait(j - 1, slot, [recv[j - 1].at[slot, d] for d in (0, 1)])
            return own(s.p)[...] + recv[j - 1][slot, 0].astype(F32) + recv[j - 1][slot, 1].astype(F32)

        return start, middle, last

    def at_stage(k, every=1):
        def run(fn):
            c = t - LAG * k
            on = (c >= 0) & (c < total)
            if every > 1:
                on &= lax.rem(c, every) == every - 1
            pl.when(on)(functools.partial(fn, c))

        return run

    def columns(c):
        return pl.ds(pl.multiple_of(lax.rem(c, chunks) * f, f), f)

    def layer_of(c):
        return 1 - lax.div(c, chunks)

    @pl.when(t == 0)
    def _():
        meet(neighbour)
        dh[1] = dy[...]
        da[...] = jnp.zeros_like(da)

    def wide(which, own, acc2, acc3, recv, stage, out):
        def own1(slot):
            return (lambda q: own.at[slot, q]) if which == "g" else (lambda q: own.at[slot, :, q])

        def p1(c):
            slot = lax.rem(c, SLOTS)
            return first(which + "1", slot, own1(slot), recv[0:2])

        def p2(c):
            slot = lax.rem(c, SLOTS)
            return later(which + "2", slot, lambda q: acc2.at[slot, q], recv[2:4], stage[0:2])

        def p3(c):
            slot, long = lax.rem(c, SLOTS), lax.rem(c, 2 * SLOTS)
            return later(which + "3", slot, lambda q: acc3.at[long, q], recv[4:8], stage[2:6])

        def end(c):
            out[layer_of(c), :, columns(c)] = p3(c)[2]()

        at_stage(8)(end)
        for j in (3, 2, 1):
            at_stage(4 + j)(lambda c, j=j: p3(c)[1](j))

        def turn2(c):
            done = p2(c)[2]()
            rows = acc3.shape[2]
            for q in range(nz):
                acc3[lax.rem(c, 2 * SLOTS), q] = done[q * rows:(q + 1) * rows]
            p3(c)[0]()

        at_stage(4)(turn2)
        at_stage(3)(lambda c: p2(c)[1](1))

        def turn1(c):
            done = p1(c)[2]()
            acc2[lax.rem(c, SLOTS)] = done.reshape(acc2.shape[1:])
            p2(c)[0]()

        at_stage(2)(turn1)
        at_stage(1)(lambda c: p1(c)[1](1))

    wide("g", own_g, acc_g2, acc_g3, rg, sg, out_g)
    wide("u", own_u, acc_u2, acc_u3, ru, su, out_u)

    def d1(c):
        slot, long = lax.rem(c, SLOTS), lax.rem(c, 2 * SLOTS)
        return first("d1", slot, lambda q: own_d.at[long, q], rd[0:4])

    def d2(c):
        slot = lax.rem(lax.div(c, ny), 2)
        return later("d2", slot, lambda q: acc_d2.at[slot, q], rd[4:6], sd[0:2])

    def d3(c):
        slot = layer_of(c)
        return later("d3", slot, lambda q: acc_d3.at[slot, q], rd[6:8], sd[2:4])

    def d_end(c):
        out_d[layer_of(c)] = d3(c)[2]()

    at_stage(8, chunks)(d_end)
    at_stage(7, chunks)(lambda c: d3(c)[1](1))

    def d_turn2(c):
        acc_d3[layer_of(c), lax.rem(lax.div(c, ny), nx)] = d2(c)[2]()

    at_stage(6, ny)(d_turn2)
    at_stage(6, chunks)(lambda c: d3(c)[0]())
    at_stage(5, ny)(lambda c: d2(c)[1](1))

    def d_turn1(c):
        acc_d2[lax.rem(lax.div(c, ny), 2), lax.rem(c, ny)] = d1(c)[2]()

    at_stage(4)(d_turn1)
    at_stage(4, ny)(lambda c: d2(c)[0]())
    for j in (3, 2, 1):
        at_stage(j)(lambda c, j=j: d1(c)[1](j))

    @pl.when(t == chunks)
    def _():
        h, by_a = h1[...].astype(F32), da[...].astype(BF).astype(F32)
        scale = lax.rsqrt(jnp.mean(h**2, -1, keepdims=True) + 1e-6)
        by_h = scale * by_a - h * (scale**3 * jnp.mean(by_a * h, -1, keepdims=True))
        dh[0] = dy[...] + by_h.astype(BF)

    def produce(c):
        g, u, d = compute(layer_of(c), 4, a_all, at_all, dh, wg, wu, wd, hid, dgate, dup, da)
        slot, long = lax.rem(c, SLOTS), lax.rem(c, 2 * SLOTS)
        own_g[slot] = g.astype(BF).reshape(own_g.shape[1:])
        own_u[slot] = u.astype(BF).reshape(own_u.shape[1:])
        own_d[long] = d.astype(BF).reshape(own_d.shape[1:])
        p = lax.rem(c, SLOTS)
        first("g1", p, lambda q: own_g.at[slot, q], rg[0:2])[0]()
        first("u1", p, lambda q: own_u.at[slot, :, q], ru[0:2])[0]()
        first("d1", p, lambda q: own_d.at[long, q], rd[0:4])[0]()

    at_stage(0)(produce)


def gradients(x, dy, wg, wu, wd):
    nx, ny, nz = GRID
    n = nx * ny * nz
    tokens, d = x.shape
    ff = wg.shape[2]
    chunks = nx * ny
    f, rg, rd = ff // chunks, d // n, ff // n
    a_all, at_all, h1 = forward(x, wg, wu, wd)
    total = 2 * chunks

    def chunk(t):
        c = t - lax.div(t, total) * (t - total + 1)
        return 1 - lax.div(c, chunks), lax.rem(c, chunks)

    def cols(t):
        layer, c = chunk(t)
        return layer, 0, c

    def rows(t):
        layer, c = chunk(t)
        return layer, c, 0

    def wide_recv(outer, inner):
        a, b = outer
        r1 = [(a // 2, b), (a, b)]
        return r1

    s, long = SLOTS, 2 * SLOTS
    g_blocks = [((ny * nz * rg) // 2, f), (ny * nz * rg, f), (nz * rg // 2, f), (nz * rg, f), (rg, f // 2), (rg, f), (rg, f), (rg, f)]
    u_blocks = [(nx // 2, nz * rg, f), (nx, nz * rg, f), (nz * rg // 2, f), (nz * rg, f), (rg, f // 2), (rg, f), (rg, f), (rg, f)]
    if nz == 4:
        g_blocks, u_blocks = g_blocks[:6], u_blocks[:6]
    d_blocks = [(rd // 2, d)] + [(rd, d)] * (nz // 2 - 1) + [(rd // 2, d), (rd, d)] * 2
    d_slots = [s] * (nz // 2) + [2] * 4
    steps = {"g1": nx, "g2": ny, "g3": nz, "u1": ny, "u2": nx, "u3": nz, "d1": nz, "d2": ny, "d3": nx}
    dma = pltpu.SemaphoreType.DMA

    def sems(name, n):
        count = 2 if name in ("d2", "d3") else s
        return (dma((n // 2, count, 2)), dma((n // 2, count, 2)))

    scratch = [
        pltpu.VMEM((tokens, f), BF), pltpu.VMEM((tokens, f), BF), pltpu.VMEM((tokens, f), BF),
        pltpu.VMEM((tokens, d), F32), pltpu.VMEM((2, tokens, d), BF),
        pltpu.VMEM((s, nx, ny * nz * rg, f), BF), pltpu.VMEM((s, nx, ny, nz * rg, f), BF), pltpu.VMEM((long, nz, rd, d), BF),
        pltpu.VMEM((s, ny, nz * rg, f), F32), pltpu.VMEM((s, nx, nz * rg, f), F32),
        pltpu.VMEM((long, nz, rg, f), F32), pltpu.VMEM((long, nz, rg, f), F32),
        pltpu.VMEM((2, ny, rd, d), F32), pltpu.VMEM((2, nx, rd, d), F32),
        [pltpu.VMEM((s, 2, *b), BF) for b in g_blocks],
        [pltpu.VMEM((s, 2, *b), BF) for b in u_blocks],
        [pltpu.VMEM((k, 2, *b), BF) for k, b in zip(d_slots, d_blocks, strict=True)],
        [pltpu.VMEM((s, 2, *b), BF) for b in g_blocks[2:]],
        [pltpu.VMEM((s, 2, *b), BF) for b in u_blocks[2:]],
        [pltpu.VMEM((k, 2, *b), BF) for k, b in zip(d_slots[nz // 2:], d_blocks[nz // 2:], strict=True)],
        [sems(name, n) for name, n in steps.items()],
    ]
    vmem = pl.BlockSpec(memory_space=pltpu.VMEM)
    return pl.pallas_call(
        reduce_kernel,
        grid=(total + 8 * LAG,),
        in_specs=[vmem] * 4 + [pl.BlockSpec((1, d, f), cols), pl.BlockSpec((1, d, f), cols), pl.BlockSpec((1, f, d), rows)],
        out_specs=[vmem] * 3,
        out_shape=[jax.ShapeDtypeStruct((2, rg, ff), F32)] * 2 + [jax.ShapeDtypeStruct((2, rd, d), F32)],
        scratch_shapes=scratch,
        compiler_params=pltpu.CompilerParams(
            vmem_limit_bytes=VMEM_LIMIT, collective_id=0, has_side_effects=True, dimension_semantics=("arbitrary",)
        ),
        name="reduce",
    )(a_all, at_all, dy, h1, wg, wu, wd)


def gather_kernel(jobs, ng, nu, nd, og, ou, od, *scratch):
    zg, zu, yg, yu, local, sems = scratch
    nx, ny, nz = GRID
    total = 2 * jobs
    f = zg.shape[-1]
    r = nd.shape[1] // jobs
    at, neighbour = place()
    x_, y_, z_ = at
    meet(neighbour)
    names = (("g1", 2), ("g2", 1), ("g3", 0), ("u1", 2), ("u2", 0), ("u3", 1), ("d1", 0), ("d2", 1), ("d3", 2))
    senders = {name: Sender(axis, at, neighbour, *sem) for (name, axis), sem in zip(names, sems, strict=True)}

    def piece(j):
        return 1 - lax.div(j, jobs), lax.rem(j, jobs)

    def blocks(name, j, slot):
        layer, q = piece(j)
        cols = pl.ds(pl.multiple_of(q * f, f), f)
        rows = pl.ds(pl.multiple_of(q * r, r), r)
        zs = lax.rem(j, 2 * SLOTS)
        h = nz * ng.shape[1] // 2
        return {
            "g1": (lambda b: zg.at[zs, b], lambda b: (zg.at[zs, b, :, pl.ds(0, f // 2)], zg.at[zs, b, :, pl.ds(f // 2, f // 2)])),
            "u1": (lambda b: zu.at[zs, b], lambda b: (zu.at[zs, b, :, pl.ds(0, f // 2)], zu.at[zs, b, :, pl.ds(f // 2, f // 2)])),
            "g2": (lambda b: og.at[layer, x_, b, :, cols], lambda b: (og.at[layer, x_, b, pl.ds(0, h), cols], og.at[layer, x_, b, pl.ds(h, h), cols])),
            "u2": (lambda b: ou.at[layer, b, y_, :, cols], lambda b: (ou.at[layer, b, y_, pl.ds(0, h), cols], ou.at[layer, b, y_, pl.ds(h, h), cols])),
            "g3": (lambda b: og.at[layer, b, :, :, cols], lambda b: (og.at[layer, b, pl.ds(0, ny // 2), :, cols], og.at[layer, b, pl.ds(ny // 2, ny // 2), :, cols])),
            "u3": (lambda b: ou.at[layer, :, b, :, cols], lambda b: (ou.at[layer, pl.ds(0, nx // 2), b, :, cols], ou.at[layer, pl.ds(nx // 2, nx // 2), b, :, cols])),
            "d1": (lambda b: od.at[layer, b, y_, z_, rows], lambda b: (od.at[layer, b, y_, z_, pl.ds(q * r, r // 2)], od.at[layer, b, y_, z_, pl.ds(q * r + r // 2, r // 2)])),
            "d2": (lambda b: od.at[layer, :, b, z_, rows], lambda b: (od.at[layer, pl.ds(0, nx // 2), b, z_, rows], od.at[layer, pl.ds(nx // 2, nx // 2), b, z_, rows])),
            "d3": (lambda b: od.at[layer, :, :, b, rows], lambda b: (od.at[layer, pl.ds(0, nx // 2), :, b, rows], od.at[layer, pl.ds(nx // 2, nx // 2), :, b, rows])),
        }[name]

    def ring(name, j, i, first=None):
        slot = lax.rem(j, SLOTS)
        s = senders[name]
        full, half = blocks(name, j, slot)
        if i > 0:
            arrived(name, j, i - 1)
        for d in (0, 1):
            b = s.block(-i if d == 0 else i)
            dst = full(b) if i < s.n // 2 - 1 else half(b)[d]
            s.copy(i, slot, d, first if first is not None else dst, dst).start()

    def arrived(name, j, i):
        slot = lax.rem(j, SLOTS)
        s = senders[name]
        full, half = blocks(name, j, slot)
        refs = []
        for d in (0, 1):
            b = s.block(-1 - i if d == 0 else 1 + i)
            refs.append(full(b) if i < s.n // 2 - 1 else half(b)[d])
        s.wait(i, slot, refs)

    def tick(t, carry):
        def at_stage(k, fn):
            j = t - LAG * k
            pl.when((j >= 0) & (j < total))(lambda: fn(j))

        def wide(which, new, zb, yb, which_local):
            p1, p2, p3 = (which + k for k in "123")

            def keep(j):
                slot = lax.rem(j, SLOTS)
                own = blocks(p2, j, slot)[0](y_ if which == "g" else x_)
                return pltpu.make_async_copy(yb.at[slot], own, local.at[which_local, slot])

            def begin(j):
                layer, q = piece(j)
                zb[lax.rem(j, 2 * SLOTS), z_] = new[layer, :, pl.ds(pl.multiple_of(q * f, f), f)]
                ring(p1, j, 0)

            def turn(j):
                slot = lax.rem(j, SLOTS)
                arrived(p1, j, nz // 2 - 1)
                yb[slot] = zb[lax.rem(j, 2 * SLOTS)].reshape(yb.shape[1:])
                keep(j).start()
                ring(p2, j, 0, yb.at[slot])

            def turn2(j):
                arrived(p2, j, 1)
                keep(j).wait()
                ring(p3, j, 0)

            k = nz // 2
            at_stage(k + 4, lambda j: arrived(p3, j, 1))
            at_stage(k + 3, lambda j: ring(p3, j, 1))
            at_stage(k + 2, turn2)
            at_stage(k + 1, lambda j: ring(p2, j, 1))
            at_stage(k, turn)
            for i in range(k - 1, 0, -1):
                at_stage(i, lambda j, i=i: ring(p1, j, i))
            at_stage(0, begin)

        wide("g", ng, zg, yg, 0)
        wide("u", nu, zu, yu, 1)

        def keep(j):
            slot = lax.rem(j, SLOTS)
            layer, q = piece(j)
            own = nd.at[layer, pl.ds(pl.multiple_of(q * r, r), r)]
            return own, pltpu.make_async_copy(own, blocks("d1", j, slot)[0](x_), local.at[2, slot])

        def d_begin(j):
            own, copy = keep(j)
            copy.start()
            ring("d1", j, 0, own)

        def d_turn(j):
            arrived("d1", j, 1)
            keep(j)[1].wait()
            ring("d2", j, 0)

        def d_turn2(j):
            arrived("d2", j, 1)
            ring("d3", j, 0)

        k = nz // 2
        at_stage(4 + k, lambda j: arrived("d3", j, k - 1))
        for i in range(k - 1, 0, -1):
            at_stage(4 + i, lambda j, i=i: ring("d3", j, i))
        at_stage(4, d_turn2)
        at_stage(3, lambda j: ring("d2", j, 1))
        at_stage(2, d_turn)
        at_stage(1, lambda j: ring("d1", j, 1))
        at_stage(0, d_begin)
        return carry

    lax.fori_loop(0, total + LAG * (nz // 2 + 4), tick, 0)


def gather(ng, nu, nd):
    nx, ny, nz = GRID
    _, rg, ff = ng.shape
    _, rd, d = nd.shape
    f = ff // JOBS
    dma = pltpu.SemaphoreType.DMA
    steps = (nz, ny, nx, nz, nx, ny, nx, ny, nz)
    wide = jax.ShapeDtypeStruct((2, nx, ny, nz * rg, ff), BF)
    og, ou, od = pl.pallas_call(
        functools.partial(gather_kernel, JOBS),
        in_specs=[pl.BlockSpec(memory_space=pltpu.VMEM)] * 3,
        out_specs=[pl.BlockSpec(memory_space=pl.ANY)] * 3,
        out_shape=[wide, wide, jax.ShapeDtypeStruct((2, nx, ny, nz, rd, d), BF)],
        scratch_shapes=[
            pltpu.VMEM((2 * SLOTS, nz, rg, f), BF), pltpu.VMEM((2 * SLOTS, nz, rg, f), BF),
            pltpu.VMEM((SLOTS, nz * rg, f), BF), pltpu.VMEM((SLOTS, nz * rg, f), BF),
            dma((3, SLOTS)),
            [(dma((n // 2, SLOTS, 2)), dma((n // 2, SLOTS, 2))) for n in steps],
        ],
        compiler_params=pltpu.CompilerParams(vmem_limit_bytes=VMEM_LIMIT, collective_id=1, has_side_effects=True),
        name="gather",
    )(ng, nu, nd)
    n = nx * ny * nz
    return og.reshape(2, n * rg, ff), ou.reshape(2, n * rg, ff), od.reshape(2, n * rd, d)


def adamw(w, m, v, g):
    g = lax.reduce_precision(g, 8, 7)
    m = 0.9 * m + 0.1 * g
    v = 0.95 * v + 0.05 * g * g
    step = m * lax.rsqrt(v + 1e-8) + 0.1 * w
    return (w - 0.02 * step).astype(BF), m, v


def device_step(x, dy, *arrays):
    weights, ms, vs = (arrays[i:i + 3] for i in (0, 3, 6))
    sums = gradients(x[0], dy[0], *weights)
    me = lax.axis_index("dp")
    new = []
    for w, m, v, g in zip(weights, ms, vs, sums, strict=True):
        rows = m.shape[1]
        own = lax.dynamic_slice_in_dim(w, me * rows, rows, 1).astype(F32)
        new.append(adamw(own, m, v, g))
    gathered = gather(*(one[0] for one in new))
    return (*gathered, *(one[1] for one in new), *(one[2] for one in new))


def solution(mesh):
    x, w, m = P(("rep", "dp"), None, None), P(None, None, None), P(None, "dp", None)
    return jax.shard_map(
        device_step,
        mesh=mesh,
        in_specs=(x, x, w, w, w, *[m] * 6),
        out_specs=(*[P("rep", None, None)] * 3, *[P("rep", "dp", None)] * 6),
        check_vma=False,
    )
```

```python
import functools

import jax
import jax.numpy as jnp
from jax import lax
from jax.experimental import pallas as pl
from jax.experimental.pallas import tpu as pltpu
from jax.sharding import PartitionSpec as P

GRID = (4, 4, 8)
BF, F32 = jnp.bfloat16, jnp.float32
MESH = pl.DeviceIdType.MESH
VMEM_LIMIT = 66_000_000
GATHER_VMEM = 12 << 20
LAG = 2
SLOTS = 6
JOBS = 8


def dot(a, b, dims=((1,), (0,))):
    return lax.dot_general(a, b, (dims, ((), ())), preferred_element_type=F32)


def normed(h):
    wide = h.astype(F32)
    scale = lax.rsqrt(jnp.mean(wide**2, -1, keepdims=True) + 1e-6)
    return (wide * scale).astype(BF)


def place():
    nx, ny, nz = GRID
    me = lax.axis_index("dp")
    at = (lax.div(me, ny * nz), lax.rem(lax.div(me, nz), ny), lax.rem(me, nz))

    def neighbour(axis, step):
        c = list(at)
        c[axis] = lax.rem(at[axis] + (step + GRID[axis]), GRID[axis])
        return (c[0] * ny + c[1]) * nz + c[2]

    return at, neighbour


def meet(neighbour):
    barrier = pltpu.get_barrier_semaphore()
    for axis in range(3):
        for step in (1, -1):
            pl.semaphore_signal(barrier, inc=1, device_id={"dp": neighbour(axis, step)}, device_id_type=MESH)
    pl.semaphore_wait(barrier, 6)


class Sender:
    def __init__(self, axis, at, neighbour, send, recv):
        self.n, self.p = GRID[axis], at[axis]
        self.to = (neighbour(axis, 1), neighbour(axis, -1))
        self.send, self.recv = send, recv

    def block(self, step):
        return lax.rem(self.p + (step + self.n), self.n)

    def copy(self, step, slot, d, src, dst):
        return pltpu.make_async_remote_copy(
            src_ref=src, dst_ref=dst, send_sem=self.send.at[step, slot, d], recv_sem=self.recv.at[step, slot, d],
            device_id={"dp": self.to[d]}, device_id_type=MESH,
        )

    def wait(self, step, slot, refs):
        for d in (0, 1):
            c = self.copy(step, slot, d, refs[d], refs[d])
            c.wait_recv()
            c.wait_send()


def compute(layer, blocks, a_all, at_all, dh, wg, wu, wd, hid, dgate, dup, da):
    tokens = dgate.shape[0]
    rows = tokens // blocks
    for b in range(blocks):
        s = pl.ds(b * rows, rows)
        a = a_all[layer, s]
        gate = dot(a, wg[0])
        up = dot(a, wu[0])
        ct = dot(dh[layer, s], wd[0], ((1,), (1,))).astype(BF).astype(F32)
        sig = jax.nn.sigmoid(gate)
        silu = gate * sig
        hid[s] = (silu * up).astype(BF)
        dup[s] = (ct * silu).astype(BF)
        dgate[s] = (ct * up * (sig + silu * (1.0 - sig))).astype(BF)

    if layer == 1:
        da[...] += dot(dgate[...], wg[0], ((1,), (1,))) + dot(dup[...], wu[0], ((1,), (1,)))

    at = at_all[layer]
    return dot(at, dgate[...]), dot(at, dup[...]), dot(hid[...], dh[layer], ((0,), (0,)))


def once(on, fn):
    def body(_, carry):
        fn()
        return carry

    lax.fori_loop(0, on.astype(jnp.int32), body, 0)


def reduce_kernel(x, dy, wg, wu, wd, out_g, out_u, out_d, *scratch):
    (hid, dgate, dup, da, dh, a_all, at_all, h1,
     own_g, own_u, own_d, acc_g2, acc_u2, acc_g3, acc_u3, acc_d2, acc_d3,
     rg, ru, rd, sg, su, sd, sems) = scratch
    nx, ny, nz = GRID
    chunks = nx * ny
    total = 2 * chunks
    f = wg.shape[2]
    t = pl.program_id(0) - chunks
    at, neighbour = place()
    x_, y_, z_ = at

    senders = {
        name: Sender(axis, at, neighbour, *sem)
        for (name, axis), sem in zip(
            (("g1", 0), ("g2", 1), ("g3", 2), ("u1", 1), ("u2", 0), ("u3", 2), ("d1", 2), ("d2", 1), ("d3", 0)), sems, strict=True
        )
    }

    def halves(array, ref):
        if array in ("g1", "g2", "d1", "d2", "d3"):
            h = ref.shape[-2] // 2
            return ref.at[pl.ds(0, h)], ref.at[pl.ds(h, h)]
        if array == "u1":
            return ref.at[pl.ds(0, nx // 2)], ref.at[pl.ds(nx // 2, nx // 2)]
        if array == "u2":
            h = ref.shape[-2] // 2
            return ref.at[pl.ds(0, h)], ref.at[pl.ds(h, h)]
        h = ref.shape[-1] // 2
        return ref.at[:, pl.ds(0, h)], ref.at[:, pl.ds(h, h)]

    def first(array, slot, own, recv):
        s = senders[array]

        def start():
            for d, half in enumerate(halves(array, own(s.block(s.n // 2)))):
                s.copy(0, slot, d, half, recv[0].at[slot, d]).start()

        def middle(j):
            s.wait(j - 1, slot, [recv[j - 1].at[slot, d] for d in (0, 1)])
            q = s.n // 2 - j
            for d in (0, 1):
                block = own(s.block(q if d == 0 else -q))
                into = halves(array, block)[d] if j == 1 else block
                into[...] = (into[...].astype(F32) + recv[j - 1][slot, d].astype(F32)).astype(BF)
                s.copy(j, slot, d, block, recv[j].at[slot, d]).start()

        def last():
            j = s.n // 2
            s.wait(j - 1, slot, [recv[j - 1].at[slot, d] for d in (0, 1)])
            return own(s.p)[...].astype(F32) + recv[j - 1][slot, 0].astype(F32) + recv[j - 1][slot, 1].astype(F32)

        return start, middle, last

    def later(array, slot, own, recv, stage):
        s = senders[array]

        def start():
            for d, half in enumerate(halves(array, own(s.block(s.n // 2)))):
                stage[0][slot, d] = half[...].astype(BF)
                s.copy(0, slot, d, stage[0].at[slot, d], recv[0].at[slot, d]).start()

        def middle(j):
            s.wait(j - 1, slot, [recv[j - 1].at[slot, d] for d in (0, 1)])
            q = s.n // 2 - j
            for d in (0, 1):
                block = own(s.block(q if d == 0 else -q))
                into = halves(array, block)[d] if j == 1 else block
                into[...] = into[...] + recv[j - 1][slot, d].astype(F32)
                stage[j][slot, d] = block[...].astype(BF)
                s.copy(j, slot, d, stage[j].at[slot, d], recv[j].at[slot, d]).start()

        def last():
            j = s.n // 2
            s.wait(j - 1, slot, [recv[j - 1].at[slot, d] for d in (0, 1)])
            return own(s.p)[...] + recv[j - 1][slot, 0].astype(F32) + recv[j - 1][slot, 1].astype(F32)

        return start, middle, last

    def at_stage(k, every=1):
        def run(fn):
            c = t - LAG * k
            on = (c >= 0) & (c < total)
            if every > 1:
                on &= lax.rem(c, every) == every - 1
            pl.when(on)(functools.partial(fn, c))

        return run

    def columns(c):
        return pl.ds(pl.multiple_of(lax.rem(c, chunks) * f, f), f)

    def layer_of(c):
        return 1 - lax.div(c, chunks)

    def enter(layer, h):
        a = normed(h)
        a_all[layer] = a
        at_all[layer] = a.T

    def begin():
        meet(neighbour)
        enter(0, x[...])
        dh[1] = dy[...]
        da[...] = jnp.zeros_like(da)

    def between():
        h = x[...] + da[...].astype(BF)
        h1[...] = h
        enter(1, h)
        da[...] = jnp.zeros_like(da)

    once(t == -chunks, begin)
    once(t == 0, between)

    @pl.when(t < 0)
    def _():
        rows = hid.shape[0] // 2
        for b in range(2):
            s = pl.ds(b * rows, rows)
            gate = dot(a_all[0, s], wg[0])
            up = dot(a_all[0, s], wu[0])
            da[s] += dot((gate * jax.nn.sigmoid(gate) * up).astype(BF), wd[0])

    def wide(which, own, acc2, acc3, recv, stage, out):
        def own1(slot):
            return (lambda q: own.at[slot, q]) if which == "g" else (lambda q: own.at[slot, :, q])

        def p1(c):
            slot = lax.rem(c, SLOTS)
            return first(which + "1", slot, own1(slot), recv[0:2])

        def p2(c):
            slot = lax.rem(c, SLOTS)
            return later(which + "2", slot, lambda q: acc2.at[slot, q], recv[2:4], stage[0:2])

        def p3(c):
            slot, long = lax.rem(c, SLOTS), lax.rem(c, 2 * SLOTS)
            return later(which + "3", slot, lambda q: acc3.at[long, q], recv[4:8], stage[2:6])

        def end(c):
            out[layer_of(c), :, columns(c)] = p3(c)[2]()

        at_stage(8)(end)
        for j in (3, 2, 1):
            at_stage(4 + j)(lambda c, j=j: p3(c)[1](j))

        def turn2(c):
            done = p2(c)[2]()
            rows = acc3.shape[2]
            for q in range(nz):
                acc3[lax.rem(c, 2 * SLOTS), q] = done[q * rows:(q + 1) * rows]
            p3(c)[0]()

        at_stage(4)(turn2)
        at_stage(3)(lambda c: p2(c)[1](1))

        def turn1(c):
            done = p1(c)[2]()
            acc2[lax.rem(c, SLOTS)] = done.reshape(acc2.shape[1:])
            p2(c)[0]()

        at_stage(2)(turn1)
        at_stage(1)(lambda c: p1(c)[1](1))

    wide("g", own_g, acc_g2, acc_g3, rg, sg, out_g)
    wide("u", own_u, acc_u2, acc_u3, ru, su, out_u)

    def d1(c):
        slot, long = lax.rem(c, SLOTS), lax.rem(c, 2 * SLOTS)
        return first("d1", slot, lambda q: own_d.at[long, q], rd[0:4])

    def d2(c):
        slot = lax.rem(lax.div(c, ny), 2)
        return later("d2", slot, lambda q: acc_d2.at[slot, q], rd[4:6], sd[0:2])

    def d3(c):
        slot = layer_of(c)
        return later("d3", slot, lambda q: acc_d3.at[slot, q], rd[6:8], sd[2:4])

    def d_end(c):
        out_d[layer_of(c)] = d3(c)[2]()

    at_stage(8, chunks)(d_end)
    at_stage(7, chunks)(lambda c: d3(c)[1](1))

    def d_turn2(c):
        acc_d3[layer_of(c), lax.rem(lax.div(c, ny), nx)] = d2(c)[2]()

    at_stage(6, ny)(d_turn2)
    at_stage(6, chunks)(lambda c: d3(c)[0]())
    at_stage(5, ny)(lambda c: d2(c)[1](1))

    def d_turn1(c):
        acc_d2[lax.rem(lax.div(c, ny), 2), lax.rem(c, ny)] = d1(c)[2]()

    at_stage(4)(d_turn1)
    at_stage(4, ny)(lambda c: d2(c)[0]())
    for j in (3, 2, 1):
        at_stage(j)(lambda c, j=j: d1(c)[1](j))

    def backward_norm():
        h, by_a = h1[...].astype(F32), da[...].astype(BF).astype(F32)
        scale = lax.rsqrt(jnp.mean(h**2, -1, keepdims=True) + 1e-6)
        by_h = scale * by_a - h * (scale**3 * jnp.mean(by_a * h, -1, keepdims=True))
        dh[0] = dy[...] + by_h.astype(BF)

    once(t == chunks, backward_norm)

    def produce(c, layer):
        g, u, d = compute(layer, 4, a_all, at_all, dh, wg, wu, wd, hid, dgate, dup, da)
        slot, long = lax.rem(c, SLOTS), lax.rem(c, 2 * SLOTS)
        own_g[slot] = g.astype(BF).reshape(own_g.shape[1:])
        own_u[slot] = u.astype(BF).reshape(own_u.shape[1:])
        own_d[long] = d.astype(BF).reshape(own_d.shape[1:])
        p = lax.rem(c, SLOTS)
        first("g1", p, lambda q: own_g.at[slot, q], rg[0:2])[0]()
        first("u1", p, lambda q: own_u.at[slot, :, q], ru[0:2])[0]()
        first("d1", p, lambda q: own_d.at[long, q], rd[0:4])[0]()

    for layer in (1, 0):
        pl.when((t >= (1 - layer) * chunks) & (t < (2 - layer) * chunks))(functools.partial(produce, t, layer))


def gradients(x, dy, wg, wu, wd):
    nx, ny, nz = GRID
    n = nx * ny * nz
    tokens, d = x.shape
    ff = wg.shape[2]
    chunks = nx * ny
    f, rg, rd = ff // chunks, d // n, ff // n
    total = 2 * chunks

    def chunk(t):
        c = t - lax.div(t, 3 * chunks) * (t - 3 * chunks + 1)
        return lax.rem(lax.div(c, chunks), 2), lax.rem(c, chunks)

    def cols(t):
        layer, c = chunk(t)
        return layer, 0, c

    def rows(t):
        layer, c = chunk(t)
        return layer, c, 0

    s, long = SLOTS, 2 * SLOTS
    g_blocks = [((ny * nz * rg) // 2, f), (ny * nz * rg, f), (nz * rg // 2, f), (nz * rg, f), (rg, f // 2), (rg, f), (rg, f), (rg, f)]
    u_blocks = [(nx // 2, nz * rg, f), (nx, nz * rg, f), (nz * rg // 2, f), (nz * rg, f), (rg, f // 2), (rg, f), (rg, f), (rg, f)]
    if nz == 4:
        g_blocks, u_blocks = g_blocks[:6], u_blocks[:6]
    d_blocks = [(rd // 2, d)] + [(rd, d)] * (nz // 2 - 1) + [(rd // 2, d), (rd, d)] * 2
    d_slots = [s] * (nz // 2) + [2] * 4
    steps = {"g1": nx, "g2": ny, "g3": nz, "u1": ny, "u2": nx, "u3": nz, "d1": nz, "d2": ny, "d3": nx}
    dma = pltpu.SemaphoreType.DMA

    def sems(name, n):
        count = 2 if name in ("d2", "d3") else s
        return (dma((n // 2, count, 2)), dma((n // 2, count, 2)))

    scratch = [
        pltpu.VMEM((tokens, f), BF), pltpu.VMEM((tokens, f), BF), pltpu.VMEM((tokens, f), BF),
        pltpu.VMEM((tokens, d), F32), pltpu.VMEM((2, tokens, d), BF),
        pltpu.VMEM((2, tokens, d), BF), pltpu.VMEM((2, d, tokens), BF), pltpu.VMEM((tokens, d), BF),
        pltpu.VMEM((s, nx, ny * nz * rg, f), BF), pltpu.VMEM((s, nx, ny, nz * rg, f), BF), pltpu.VMEM((long, nz, rd, d), BF),
        pltpu.VMEM((s, ny, nz * rg, f), F32), pltpu.VMEM((s, nx, nz * rg, f), F32),
        pltpu.VMEM((long, nz, rg, f), F32), pltpu.VMEM((long, nz, rg, f), F32),
        pltpu.VMEM((2, ny, rd, d), F32), pltpu.VMEM((2, nx, rd, d), F32),
        [pltpu.VMEM((s, 2, *b), BF) for b in g_blocks],
        [pltpu.VMEM((s, 2, *b), BF) for b in u_blocks],
        [pltpu.VMEM((k, 2, *b), BF) for k, b in zip(d_slots, d_blocks, strict=True)],
        [pltpu.VMEM((s, 2, *b), BF) for b in g_blocks[2:]],
        [pltpu.VMEM((s, 2, *b), BF) for b in u_blocks[2:]],
        [pltpu.VMEM((k, 2, *b), BF) for k, b in zip(d_slots[nz // 2:], d_blocks[nz // 2:], strict=True)],
        [sems(name, n) for name, n in steps.items()],
    ]
    vmem = pl.BlockSpec(memory_space=pltpu.VMEM)
    return pl.pallas_call(
        reduce_kernel,
        grid=(chunks + total + 8 * LAG,),
        in_specs=[vmem] * 2 + [pl.BlockSpec((1, d, f), cols), pl.BlockSpec((1, d, f), cols), pl.BlockSpec((1, f, d), rows)],
        out_specs=[vmem] * 3,
        out_shape=[jax.ShapeDtypeStruct((2, rg, ff), F32)] * 2 + [jax.ShapeDtypeStruct((2, rd, d), F32)],
        scratch_shapes=scratch,
        compiler_params=pltpu.CompilerParams(
            vmem_limit_bytes=VMEM_LIMIT, collective_id=0, has_side_effects=True, dimension_semantics=("arbitrary",)
        ),
        name="reduce",
    )(x, dy, wg, wu, wd)


def gather_kernel(jobs, ng, nu, nd, og, ou, od, *scratch):
    zg, zu, yg, yu, local, sems = scratch
    nx, ny, nz = GRID
    total = 2 * jobs
    f = zg.shape[-1]
    r = nd.shape[1] // jobs
    at, neighbour = place()
    x_, y_, z_ = at
    meet(neighbour)
    names = (("g1", 2), ("g2", 1), ("g3", 0), ("u1", 2), ("u2", 0), ("u3", 1), ("d1", 0), ("d2", 1), ("d3", 2))
    senders = {name: Sender(axis, at, neighbour, *sem) for (name, axis), sem in zip(names, sems, strict=True)}
    senders |= {"e1": Sender(1, at, neighbour, *sems[6]), "e2": Sender(0, at, neighbour, *sems[7])}

    def piece(j):
        return 1 - lax.div(j, jobs), lax.rem(j, jobs)

    def blocks(name, j, slot):
        layer, q = piece(j)
        cols = pl.ds(pl.multiple_of(q * f, f), f)
        rows = pl.ds(pl.multiple_of(q * r, r), r)
        zs = lax.rem(j, 2 * SLOTS)
        left, right = pl.ds(0, nd.shape[2] // 2), pl.ds(nd.shape[2] // 2, nd.shape[2] // 2)
        h = nz * ng.shape[1] // 2
        return {
            "g1": (lambda b: zg.at[zs, b], lambda b: (zg.at[zs, b, :, pl.ds(0, f // 2)], zg.at[zs, b, :, pl.ds(f // 2, f // 2)])),
            "u1": (lambda b: zu.at[zs, b], lambda b: (zu.at[zs, b, :, pl.ds(0, f // 2)], zu.at[zs, b, :, pl.ds(f // 2, f // 2)])),
            "g2": (lambda b: og.at[layer, x_, b, :, cols], lambda b: (og.at[layer, x_, b, pl.ds(0, h), cols], og.at[layer, x_, b, pl.ds(h, h), cols])),
            "u2": (lambda b: ou.at[layer, b, y_, :, cols], lambda b: (ou.at[layer, b, y_, pl.ds(0, h), cols], ou.at[layer, b, y_, pl.ds(h, h), cols])),
            "g3": (lambda b: og.at[layer, b, :, :, cols], lambda b: (og.at[layer, b, pl.ds(0, ny // 2), :, cols], og.at[layer, b, pl.ds(ny // 2, ny // 2), :, cols])),
            "u3": (lambda b: ou.at[layer, :, b, :, cols], lambda b: (ou.at[layer, pl.ds(0, nx // 2), b, :, cols], ou.at[layer, pl.ds(nx // 2, nx // 2), b, :, cols])),
            "d1": (lambda b: od.at[layer, b, y_, z_, rows], lambda b: (od.at[layer, b, y_, z_, rows, left], od.at[layer, b, y_, z_, rows, right])),
            "e1": (lambda b: od.at[layer, x_, b, z_, rows], lambda b: (od.at[layer, x_, b, z_, rows, left], od.at[layer, x_, b, z_, rows, right])),
            "d2": (lambda b: od.at[layer, :, b, z_, rows], lambda b: (od.at[layer, pl.ds(0, nx // 2), b, z_, rows], od.at[layer, pl.ds(nx // 2, nx // 2), b, z_, rows])),
            "e2": (lambda b: od.at[layer, b, :, z_, rows], lambda b: (od.at[layer, b, pl.ds(0, ny // 2), z_, rows], od.at[layer, b, pl.ds(ny // 2, ny // 2), z_, rows])),
            "d3": (lambda b: od.at[layer, :, :, b, rows], lambda b: (od.at[layer, pl.ds(0, nx // 2), :, b, rows], od.at[layer, pl.ds(nx // 2, nx // 2), :, b, rows])),
        }[name]

    def ring(name, j, i, first=None):
        slot = lax.rem(j, SLOTS)
        s = senders[name]
        full, half = blocks(name, j, slot)
        if i > 0:
            arrived(name, j, i - 1)
        for d in (0, 1):
            b = s.block(-i if d == 0 else i)
            dst = full(b) if i < s.n // 2 - 1 else half(b)[d]
            s.copy(i, slot, d, first if first is not None else dst, dst).start()

    def arrived(name, j, i):
        slot = lax.rem(j, SLOTS)
        s = senders[name]
        full, half = blocks(name, j, slot)
        refs = []
        for d in (0, 1):
            b = s.block(-1 - i if d == 0 else 1 + i)
            refs.append(full(b) if i < s.n // 2 - 1 else half(b)[d])
        s.wait(i, slot, refs)

    def tick(t, carry):
        def at_stage(k, fn):
            j = t - LAG * k
            pl.when((j >= 0) & (j < total))(lambda: fn(j))

        def wide(which, new, zb, yb, which_local):
            p1, p2, p3 = (which + k for k in "123")

            def keep(j):
                slot = lax.rem(j, SLOTS)
                own = blocks(p2, j, slot)[0](y_ if which == "g" else x_)
                return pltpu.make_async_copy(yb.at[slot], own, local.at[which_local, slot])

            def begin(j):
                layer, q = piece(j)
                zb[lax.rem(j, 2 * SLOTS), z_] = new[layer, :, pl.ds(pl.multiple_of(q * f, f), f)]
                ring(p1, j, 0)

            def turn(j):
                slot = lax.rem(j, SLOTS)
                arrived(p1, j, nz // 2 - 1)
                yb[slot] = zb[lax.rem(j, 2 * SLOTS)].reshape(yb.shape[1:])
                keep(j).start()
                ring(p2, j, 0, yb.at[slot])

            def turn2(j):
                arrived(p2, j, 1)
                keep(j).wait()
                ring(p3, j, 0)

            k = nz // 2
            at_stage(k + 4, lambda j: arrived(p3, j, 1))
            at_stage(k + 3, lambda j: ring(p3, j, 1))
            at_stage(k + 2, turn2)
            at_stage(k + 1, lambda j: ring(p2, j, 1))
            at_stage(k, turn)
            for i in range(k - 1, 0, -1):
                at_stage(i, lambda j, i=i: ring(p1, j, i))
            at_stage(0, begin)

        wide("g", ng, zg, yg, 0)
        wide("u", nu, zu, yu, 1)

        def keep(j):
            slot = lax.rem(j, SLOTS)
            layer, q = piece(j)
            own = nd.at[layer, pl.ds(pl.multiple_of(q * r, r), r)]
            return own, pltpu.make_async_copy(own, blocks("d1", j, slot)[0](x_), local.at[2, slot])

        def d_begin(name, j):
            own, copy = keep(j)
            copy.start()
            ring(name + "1", j, 0, own)

        def d_turn(name, j):
            arrived(name + "1", j, 1)
            keep(j)[1].wait()
            ring(name + "2", j, 0)

        def d_turn2(name, j):
            arrived(name + "2", j, 1)
            ring("d3", j, 0)

        def either(k, fn):
            at_stage(k, lambda j: pl.when(lax.rem(j, 2) == 0)(lambda: fn("d", j)))
            at_stage(k, lambda j: pl.when(lax.rem(j, 2) == 1)(lambda: fn("e", j)))

        k = nz // 2
        at_stage(4 + k, lambda j: arrived("d3", j, k - 1))
        for i in range(k - 1, 0, -1):
            at_stage(4 + i, lambda j, i=i: ring("d3", j, i))
        either(4, d_turn2)
        either(3, lambda name, j: ring(name + "2", j, 1))
        either(2, d_turn)
        either(1, lambda name, j: ring(name + "1", j, 1))
        either(0, d_begin)
        return carry

    lax.fori_loop(0, total + LAG * (nz // 2 + 4), tick, 0)


def gather(ng, nu, nd):
    nx, ny, nz = GRID
    _, rg, ff = ng.shape
    _, rd, d = nd.shape
    f = ff // JOBS
    dma = pltpu.SemaphoreType.DMA
    steps = (nz, ny, nx, nz, nx, ny, nx, ny, nz)
    wide = jax.ShapeDtypeStruct((2, nx, ny, nz * rg, ff), BF)
    og, ou, od = pl.pallas_call(
        functools.partial(gather_kernel, JOBS),
        in_specs=[pl.BlockSpec(memory_space=pltpu.VMEM)] * 3,
        out_specs=[pl.BlockSpec(memory_space=pl.ANY)] * 3,
        out_shape=[wide, wide, jax.ShapeDtypeStruct((2, nx, ny, nz, rd, d), BF)],
        scratch_shapes=[
            pltpu.VMEM((2 * SLOTS, nz, rg, f), BF), pltpu.VMEM((2 * SLOTS, nz, rg, f), BF),
            pltpu.VMEM((SLOTS, nz * rg, f), BF), pltpu.VMEM((SLOTS, nz * rg, f), BF),
            dma((3, SLOTS)),
            [(dma((n // 2, SLOTS, 2)), dma((n // 2, SLOTS, 2))) for n in steps],
        ],
        compiler_params=pltpu.CompilerParams(vmem_limit_bytes=GATHER_VMEM, collective_id=1, has_side_effects=True),
        name="gather",
    )(ng, nu, nd)
    n = nx * ny * nz
    return og.reshape(2, n * rg, ff), ou.reshape(2, n * rg, ff), od.reshape(2, n * rd, d)


def adamw(w, m, v, g):
    g = lax.reduce_precision(g, 8, 7)
    m = 0.9 * m + 0.1 * g
    v = 0.95 * v + 0.05 * g * g
    step = m * lax.rsqrt(v + 1e-8) + 0.1 * w
    return (w - 0.02 * step).astype(BF), m, v


def device_step(x, dy, *arrays):
    weights, ms, vs = (arrays[i:i + 3] for i in (0, 3, 6))
    sums = gradients(x[0], dy[0], *weights)
    me = lax.axis_index("dp")
    new = []
    for w, m, v, g in zip(weights, ms, vs, sums, strict=True):
        rows = m.shape[1]
        own = lax.dynamic_slice_in_dim(w, me * rows, rows, 1).astype(F32)
        new.append(adamw(own, m, v, g))
    gathered = gather(*(one[0] for one in new))
    return (*gathered, *(one[1] for one in new), *(one[2] for one in new))


def solution(mesh):
    x, w, m = P(("rep", "dp"), None, None), P(None, None, None), P(None, "dp", None)
    return jax.shard_map(
        device_step,
        mesh=mesh,
        in_specs=(x, x, w, w, w, *[m] * 6),
        out_specs=(*[P("rep", None, None)] * 3, *[P("rep", "dp", None)] * 6),
        check_vma=False,
    )
```

```python
import functools

import jax
import jax.numpy as jnp
from jax import lax
from jax.experimental import pallas as pl
from jax.experimental.pallas import tpu as pltpu
from jax.sharding import PartitionSpec as P

GRID = (4, 4, 8)
BF, F32 = jnp.bfloat16, jnp.float32
MESH = pl.DeviceIdType.MESH
VMEM_LIMIT = 66_000_000
GATHER_VMEM = 12 << 20
LAG = 2
SLOTS = 6
GROUPS = 3
JOBS = 4
GATHER_LAG = 3


def dot(a, b, dims=((1,), (0,))):
    return lax.dot_general(a, b, (dims, ((), ())), preferred_element_type=F32)


def normed(h):
    wide = h.astype(F32)
    scale = lax.rsqrt(jnp.mean(wide**2, -1, keepdims=True) + 1e-6)
    return (wide * scale).astype(BF)


def place():
    nx, ny, nz = GRID
    me = lax.axis_index("dp")
    at = (lax.div(me, ny * nz), lax.rem(lax.div(me, nz), ny), lax.rem(me, nz))

    def neighbour(axis, step):
        c = list(at)
        c[axis] = lax.rem(at[axis] + (step + GRID[axis]), GRID[axis])
        return (c[0] * ny + c[1]) * nz + c[2]

    return at, neighbour


def meet(neighbour):
    barrier = pltpu.get_barrier_semaphore()
    for axis in range(3):
        for step in (1, -1):
            pl.semaphore_signal(barrier, inc=1, device_id={"dp": neighbour(axis, step)}, device_id_type=MESH)
    pl.semaphore_wait(barrier, 6)


class Sender:
    def __init__(self, axis, at, neighbour, send, recv):
        self.n, self.p = GRID[axis], at[axis]
        self.to = (neighbour(axis, 1), neighbour(axis, -1))
        self.send, self.recv = send, recv

    def block(self, step):
        return lax.rem(self.p + (step + self.n), self.n)

    def copy(self, step, slot, d, src, dst):
        return pltpu.make_async_remote_copy(
            src_ref=src, dst_ref=dst, send_sem=self.send.at[step, slot, d], recv_sem=self.recv.at[step, slot, d],
            device_id={"dp": self.to[d]}, device_id_type=MESH,
        )

    def wait(self, step, slot, refs):
        for d in (0, 1):
            c = self.copy(step, slot, d, refs[d], refs[d])
            c.wait_recv()
            c.wait_send()


def compute(layer, blocks, a_all, at_all, dh, wg, wu, wd, hid, dgate, dup, da):
    tokens = dgate.shape[0]
    rows = tokens // blocks
    for b in range(blocks):
        s = pl.ds(b * rows, rows)
        a = a_all[layer, s]
        gate = dot(a, wg[0])
        up = dot(a, wu[0])
        ct = dot(dh[layer, s], wd[0], ((1,), (1,))).astype(BF).astype(F32)
        sig = jax.nn.sigmoid(gate)
        silu = gate * sig
        hid[s] = (silu * up).astype(BF)
        dup[s] = (ct * silu).astype(BF)
        dgate[s] = (ct * up * (sig + silu * (1.0 - sig))).astype(BF)

    if layer == 1:
        da[...] += dot(dgate[...], wg[0], ((1,), (1,))) + dot(dup[...], wu[0], ((1,), (1,)))

    at = at_all[layer]
    return dot(at, dgate[...]), dot(at, dup[...]), dot(hid[...], dh[layer], ((0,), (0,)))


def once(on, fn):
    def body(_, carry):
        fn()
        return carry

    lax.fori_loop(0, on.astype(jnp.int32), body, 0)


def reduce_kernel(x, dy, wg, wu, wd, out_g, out_u, out_d, *scratch):
    (hid, dgate, dup, da, dh, a_all, at_all, h1,
     own_g, own_u, own_d, acc_g2, acc_u2, acc_w3, acc_d2, acc_d3,
     rg, ru, rw, rd, sg, su, sw, sd, sems) = scratch
    nx, ny, nz = GRID
    chunks = nx * ny
    total = 2 * chunks
    f = wg.shape[2]
    t = pl.program_id(0) - chunks
    at, neighbour = place()
    x_, y_, z_ = at

    senders = {
        name: Sender(axis, at, neighbour, *sem)
        for (name, axis), sem in zip(
            (("g1", 0), ("g2", 1), ("u1", 1), ("u2", 0), ("w3", 2), ("d1", 2), ("d2", 1), ("d3", 0)), sems, strict=True
        )
    }

    def halves(array, ref):
        if array == "w3":
            return ref.at[0], ref.at[1]
        h = ref.shape[0] // 2
        return ref.at[pl.ds(0, h)], ref.at[pl.ds(h, h)]

    def first(array, slot, own, recv):
        s = senders[array]

        def start():
            for d, half in enumerate(halves(array, own(s.block(s.n // 2)))):
                s.copy(0, slot, d, half, recv[0].at[slot, d]).start()

        def middle(j):
            s.wait(j - 1, slot, [recv[j - 1].at[slot, d] for d in (0, 1)])
            q = s.n // 2 - j
            for d in (0, 1):
                block = own(s.block(q if d == 0 else -q))
                into = halves(array, block)[d] if j == 1 else block
                into[...] = (into[...].astype(F32) + recv[j - 1][slot, d].astype(F32)).astype(BF)
                s.copy(j, slot, d, block, recv[j].at[slot, d]).start()

        def last():
            j = s.n // 2
            s.wait(j - 1, slot, [recv[j - 1].at[slot, d] for d in (0, 1)])
            return own(s.p)[...].astype(F32) + recv[j - 1][slot, 0].astype(F32) + recv[j - 1][slot, 1].astype(F32)

        return start, middle, last

    def later(array, slot, own, recv, stage):
        s = senders[array]

        def start():
            for d, half in enumerate(halves(array, own(s.block(s.n // 2)))):
                stage[0][slot, d] = half[...].astype(BF)
                s.copy(0, slot, d, stage[0].at[slot, d], recv[0].at[slot, d]).start()

        def middle(j):
            s.wait(j - 1, slot, [recv[j - 1].at[slot, d] for d in (0, 1)])
            q = s.n // 2 - j
            for d in (0, 1):
                block = own(s.block(q if d == 0 else -q))
                into = halves(array, block)[d] if j == 1 else block
                into[...] = into[...] + recv[j - 1][slot, d].astype(F32)
                stage[j][slot, d] = block[...].astype(BF)
                s.copy(j, slot, d, stage[j].at[slot, d], recv[j].at[slot, d]).start()

        def last():
            j = s.n // 2
            s.wait(j - 1, slot, [recv[j - 1].at[slot, d] for d in (0, 1)])
            return own(s.p)[...] + recv[j - 1][slot, 0].astype(F32) + recv[j - 1][slot, 1].astype(F32)

        return start, middle, last

    def at_stage(k, every=1):
        def run(fn):
            c = t - LAG * k
            on = (c >= 0) & (c < total)
            if every > 1:
                on &= lax.rem(c, every) == every - 1
            pl.when(on)(functools.partial(fn, c))

        return run

    def layer_of(c):
        return 1 - lax.div(c, chunks)

    def enter(layer, h):
        a = normed(h)
        a_all[layer] = a
        at_all[layer] = a.T

    def begin():
        meet(neighbour)
        enter(0, x[...])
        dh[1] = dy[...]
        da[...] = jnp.zeros_like(da)

    def between():
        h = x[...] + da[...].astype(BF)
        h1[...] = h
        enter(1, h)
        da[...] = jnp.zeros_like(da)

    once(t == -chunks, begin)
    once(t == 0, between)

    @pl.when(t < 0)
    def _():
        rows = hid.shape[0] // 2
        for b in range(2):
            s = pl.ds(b * rows, rows)
            gate = dot(a_all[0, s], wg[0])
            up = dot(a_all[0, s], wu[0])
            da[s] += dot((gate * jax.nn.sigmoid(gate) * up).astype(BF), wd[0])

    def w3(c):
        slot = lax.rem(lax.div(c, ny), GROUPS)
        return later("w3", slot, lambda q: acc_w3.at[slot, q], rw, sw)

    def w_end(c):
        done = w3(c)[2]()
        cols = pl.ds(pl.multiple_of(lax.div(lax.rem(c, chunks), ny) * (ny * f), ny * f), ny * f)
        out_g[layer_of(c), :, cols] = done[0]
        out_u[layer_of(c), :, cols] = done[1]

    at_stage(8, ny)(w_end)
    for j in (3, 2, 1):
        at_stage(4 + j, ny)(lambda c, j=j: w3(c)[1](j))

    def wide(which, own, acc2, recv, stage):
        def own1(slot):
            return (lambda q: own.at[slot, q]) if which == "g" else (lambda q: own.at[slot, :, q])

        def p1(c):
            slot = lax.rem(c, SLOTS)
            return first(which + "1", slot, own1(slot), recv[0:2])

        def p2(c):
            slot = lax.rem(c, SLOTS)
            return later(which + "2", slot, lambda q: acc2.at[slot, q], recv[2:4], stage[0:2])

        def turn2(c):
            done = p2(c)[2]()
            rows = acc_w3.shape[3]
            cols = pl.ds(pl.multiple_of(lax.rem(c, ny) * f, f), f)
            for q in range(nz):
                acc_w3[lax.rem(lax.div(c, ny), GROUPS), q, "gu".index(which), :, cols] = done[q * rows:(q + 1) * rows]

        at_stage(4)(turn2)
        at_stage(3)(lambda c: p2(c)[1](1))

        def turn1(c):
            done = p1(c)[2]()
            acc2[lax.rem(c, SLOTS)] = done.reshape(acc2.shape[1:])
            p2(c)[0]()

        at_stage(2)(turn1)
        at_stage(1)(lambda c: p1(c)[1](1))

    wide("g", own_g, acc_g2, rg, sg)
    wide("u", own_u, acc_u2, ru, su)
    at_stage(4, ny)(lambda c: w3(c)[0]())

    def d1(c):
        slot, long = lax.rem(c, SLOTS), lax.rem(c, 2 * SLOTS)
        return first("d1", slot, lambda q: own_d.at[long, q], rd[0:4])

    def d2(c):
        slot = lax.rem(lax.div(c, ny), 2)
        return later("d2", slot, lambda q: acc_d2.at[slot, q], rd[4:6], sd[0:2])

    def d3(c):
        slot = layer_of(c)
        return later("d3", slot, lambda q: acc_d3.at[slot, q], rd[6:8], sd[2:4])

    def d_end(c):
        out_d[layer_of(c)] = d3(c)[2]()

    at_stage(8, chunks)(d_end)
    at_stage(7, chunks)(lambda c: d3(c)[1](1))

    def d_turn2(c):
        acc_d3[layer_of(c), lax.rem(lax.div(c, ny), nx)] = d2(c)[2]()

    at_stage(6, ny)(d_turn2)
    at_stage(6, chunks)(lambda c: d3(c)[0]())
    at_stage(5, ny)(lambda c: d2(c)[1](1))

    def d_turn1(c):
        acc_d2[lax.rem(lax.div(c, ny), 2), lax.rem(c, ny)] = d1(c)[2]()

    at_stage(4)(d_turn1)
    at_stage(4, ny)(lambda c: d2(c)[0]())
    for j in (3, 2, 1):
        at_stage(j)(lambda c, j=j: d1(c)[1](j))

    def backward_norm():
        h, by_a = h1[...].astype(F32), da[...].astype(BF).astype(F32)
        scale = lax.rsqrt(jnp.mean(h**2, -1, keepdims=True) + 1e-6)
        by_h = scale * by_a - h * (scale**3 * jnp.mean(by_a * h, -1, keepdims=True))
        dh[0] = dy[...] + by_h.astype(BF)

    once(t == chunks, backward_norm)

    def produce(c, layer):
        g, u, d = compute(layer, 4, a_all, at_all, dh, wg, wu, wd, hid, dgate, dup, da)
        slot, long = lax.rem(c, SLOTS), lax.rem(c, 2 * SLOTS)
        own_g[slot] = g.astype(BF).reshape(own_g.shape[1:])
        own_u[slot] = u.astype(BF).reshape(own_u.shape[1:])
        own_d[long] = d.astype(BF).reshape(own_d.shape[1:])
        p = lax.rem(c, SLOTS)
        first("g1", p, lambda q: own_g.at[slot, q], rg[0:2])[0]()
        first("u1", p, lambda q: own_u.at[slot, :, q], ru[0:2])[0]()
        first("d1", p, lambda q: own_d.at[long, q], rd[0:4])[0]()

    for layer in (1, 0):
        pl.when((t >= (1 - layer) * chunks) & (t < (2 - layer) * chunks))(functools.partial(produce, t, layer))


def gradients(x, dy, wg, wu, wd):
    nx, ny, nz = GRID
    n = nx * ny * nz
    tokens, d = x.shape
    ff = wg.shape[2]
    chunks = nx * ny
    f, rg, rd = ff // chunks, d // n, ff // n
    total = 2 * chunks

    def chunk(t):
        c = t - lax.div(t, 3 * chunks) * (t - 3 * chunks + 1)
        return lax.rem(lax.div(c, chunks), 2), lax.rem(c, chunks)

    def cols(t):
        layer, c = chunk(t)
        return layer, 0, c

    def rows(t):
        layer, c = chunk(t)
        return layer, c, 0

    s, long = SLOTS, 2 * SLOTS
    g_blocks = [((ny * nz * rg) // 2, f), (ny * nz * rg, f), (nz * rg // 2, f), (nz * rg, f)]
    u_blocks = [(nx // 2, nz * rg, f), (nx, nz * rg, f), (nz * rg // 2, f), (nz * rg, f)]
    w_blocks = [(rg, ny * f)] + [(2, rg, ny * f)] * (nz // 2 - 1)
    d_blocks = [(rd // 2, d)] + [(rd, d)] * (nz // 2 - 1) + [(rd // 2, d), (rd, d)] * 2
    d_slots = [s] * (nz // 2) + [2] * 4
    steps = {"g1": nx, "g2": ny, "u1": ny, "u2": nx, "w3": nz, "d1": nz, "d2": ny, "d3": nx}
    dma = pltpu.SemaphoreType.DMA

    def sems(name, n):
        count = {"d2": 2, "d3": 2, "w3": GROUPS}.get(name, s)
        return (dma((n // 2, count, 2)), dma((n // 2, count, 2)))

    scratch = [
        pltpu.VMEM((tokens, f), BF), pltpu.VMEM((tokens, f), BF), pltpu.VMEM((tokens, f), BF),
        pltpu.VMEM((tokens, d), F32), pltpu.VMEM((2, tokens, d), BF),
        pltpu.VMEM((2, tokens, d), BF), pltpu.VMEM((2, d, tokens), BF), pltpu.VMEM((tokens, d), BF),
        pltpu.VMEM((s, nx, ny * nz * rg, f), BF), pltpu.VMEM((s, nx, ny, nz * rg, f), BF), pltpu.VMEM((long, nz, rd, d), BF),
        pltpu.VMEM((s, ny, nz * rg, f), F32), pltpu.VMEM((s, nx, nz * rg, f), F32),
        pltpu.VMEM((GROUPS, nz, 2, rg, ny * f), F32),
        pltpu.VMEM((2, ny, rd, d), F32), pltpu.VMEM((2, nx, rd, d), F32),
        [pltpu.VMEM((s, 2, *b), BF) for b in g_blocks],
        [pltpu.VMEM((s, 2, *b), BF) for b in u_blocks],
        [pltpu.VMEM((GROUPS, 2, *b), BF) for b in w_blocks],
        [pltpu.VMEM((k, 2, *b), BF) for k, b in zip(d_slots, d_blocks, strict=True)],
        [pltpu.VMEM((s, 2, *b), BF) for b in g_blocks[2:]],
        [pltpu.VMEM((s, 2, *b), BF) for b in u_blocks[2:]],
        [pltpu.VMEM((GROUPS, 2, *b), BF) for b in w_blocks],
        [pltpu.VMEM((k, 2, *b), BF) for k, b in zip(d_slots[nz // 2:], d_blocks[nz // 2:], strict=True)],
        [sems(name, n) for name, n in steps.items()],
    ]
    vmem = pl.BlockSpec(memory_space=pltpu.VMEM)
    return pl.pallas_call(
        reduce_kernel,
        grid=(chunks + total + 8 * LAG,),
        in_specs=[vmem] * 2 + [pl.BlockSpec((1, d, f), cols), pl.BlockSpec((1, d, f), cols), pl.BlockSpec((1, f, d), rows)],
        out_specs=[vmem] * 3,
        out_shape=[jax.ShapeDtypeStruct((2, rg, ff), F32)] * 2 + [jax.ShapeDtypeStruct((2, rd, d), F32)],
        scratch_shapes=scratch,
        compiler_params=pltpu.CompilerParams(
            vmem_limit_bytes=VMEM_LIMIT, collective_id=0, has_side_effects=True, dimension_semantics=("arbitrary",)
        ),
        name="reduce",
    )(x, dy, wg, wu, wd)


def gather_kernel(jobs, ng, nu, nd, og, ou, od, *scratch):
    zg, zu, yg, yu, local, sems = scratch
    nx, ny, nz = GRID
    total = 2 * jobs
    f = zg.shape[-1]
    r = nd.shape[1] // jobs
    at, neighbour = place()
    x_, y_, z_ = at
    meet(neighbour)
    names = (("g1", 2), ("g2", 1), ("g3", 0), ("u1", 2), ("u2", 0), ("u3", 1), ("d1", 0), ("d2", 1), ("d3", 2))
    senders = {name: Sender(axis, at, neighbour, *sem) for (name, axis), sem in zip(names, sems, strict=True)}
    senders |= {"e1": Sender(1, at, neighbour, *sems[6]), "e2": Sender(0, at, neighbour, *sems[7])}

    def piece(j):
        return 1 - lax.div(j, jobs), lax.rem(j, jobs)

    def blocks(name, j, slot):
        layer, q = piece(j)
        cols = pl.ds(pl.multiple_of(q * f, f), f)
        rows = pl.ds(pl.multiple_of(q * r, r), r)
        zs = j
        left, right = pl.ds(0, nd.shape[2] // 2), pl.ds(nd.shape[2] // 2, nd.shape[2] // 2)
        h = nz * ng.shape[1] // 2
        return {
            "g1": (lambda b: zg.at[zs, b], lambda b: (zg.at[zs, b, :, pl.ds(0, f // 2)], zg.at[zs, b, :, pl.ds(f // 2, f // 2)])),
            "u1": (lambda b: zu.at[zs, b], lambda b: (zu.at[zs, b, :, pl.ds(0, f // 2)], zu.at[zs, b, :, pl.ds(f // 2, f // 2)])),
            "g2": (lambda b: og.at[layer, x_, b, :, cols], lambda b: (og.at[layer, x_, b, pl.ds(0, h), cols], og.at[layer, x_, b, pl.ds(h, h), cols])),
            "u2": (lambda b: ou.at[layer, b, y_, :, cols], lambda b: (ou.at[layer, b, y_, pl.ds(0, h), cols], ou.at[layer, b, y_, pl.ds(h, h), cols])),
            "g3": (lambda b: og.at[layer, b, :, :, cols], lambda b: (og.at[layer, b, pl.ds(0, ny // 2), :, cols], og.at[layer, b, pl.ds(ny // 2, ny // 2), :, cols])),
            "u3": (lambda b: ou.at[layer, :, b, :, cols], lambda b: (ou.at[layer, pl.ds(0, nx // 2), b, :, cols], ou.at[layer, pl.ds(nx // 2, nx // 2), b, :, cols])),
            "d1": (lambda b: od.at[layer, b, y_, z_, rows], lambda b: (od.at[layer, b, y_, z_, rows, left], od.at[layer, b, y_, z_, rows, right])),
            "e1": (lambda b: od.at[layer, x_, b, z_, rows], lambda b: (od.at[layer, x_, b, z_, rows, left], od.at[layer, x_, b, z_, rows, right])),
            "d2": (lambda b: od.at[layer, :, b, z_, rows], lambda b: (od.at[layer, pl.ds(0, nx // 2), b, z_, rows], od.at[layer, pl.ds(nx // 2, nx // 2), b, z_, rows])),
            "e2": (lambda b: od.at[layer, b, :, z_, rows], lambda b: (od.at[layer, b, pl.ds(0, ny // 2), z_, rows], od.at[layer, b, pl.ds(ny // 2, ny // 2), z_, rows])),
            "d3": (lambda b: od.at[layer, :, :, b, rows], lambda b: (od.at[layer, pl.ds(0, nx // 2), :, b, rows], od.at[layer, pl.ds(nx // 2, nx // 2), :, b, rows])),
        }[name]

    def ring(name, j, i, first=None):
        slot = j
        s = senders[name]
        full, half = blocks(name, j, slot)
        if i > 0:
            arrived(name, j, i - 1)
        for d in (0, 1):
            b = s.block(-i if d == 0 else i)
            dst = full(b) if i < s.n // 2 - 1 else half(b)[d]
            s.copy(i, slot, d, first if first is not None else dst, dst).start()

    def arrived(name, j, i):
        slot = j
        s = senders[name]
        full, half = blocks(name, j, slot)
        refs = []
        for d in (0, 1):
            b = s.block(-1 - i if d == 0 else 1 + i)
            refs.append(full(b) if i < s.n // 2 - 1 else half(b)[d])
        s.wait(i, slot, refs)

    def tick(t, carry):
        def at_stage(k, fn):
            j = t - GATHER_LAG * k
            pl.when((j >= 0) & (j < total))(lambda: fn(j))

        def wide(which, new, zb, yb, which_local):
            p1, p2, p3 = (which + k for k in "123")

            def keep(j):
                slot = j
                own = blocks(p2, j, slot)[0](y_ if which == "g" else x_)
                return pltpu.make_async_copy(yb.at[slot], own, local.at[which_local, slot])

            def begin(j):
                layer, q = piece(j)
                zb[j, z_] = new[layer, :, pl.ds(pl.multiple_of(q * f, f), f)]
                ring(p1, j, 0)

            def turn(j):
                slot = j
                arrived(p1, j, nz // 2 - 1)
                yb[slot] = zb[j].reshape(yb.shape[1:])
                keep(j).start()
                ring(p2, j, 0, yb.at[slot])

            def turn2(j):
                arrived(p2, j, 1)
                keep(j).wait()
                ring(p3, j, 0)

            k = nz // 2
            at_stage(k + 4, lambda j: arrived(p3, j, 1))
            at_stage(k + 3, lambda j: ring(p3, j, 1))
            at_stage(k + 2, turn2)
            at_stage(k + 1, lambda j: ring(p2, j, 1))
            at_stage(k, turn)
            for i in range(k - 1, 0, -1):
                at_stage(i, lambda j, i=i: ring(p1, j, i))
            at_stage(0, begin)

        wide("g", ng, zg, yg, 0)
        wide("u", nu, zu, yu, 1)

        def keep(j):
            slot = j
            layer, q = piece(j)
            own = nd.at[layer, pl.ds(pl.multiple_of(q * r, r), r)]
            return own, pltpu.make_async_copy(own, blocks("d1", j, slot)[0](x_), local.at[2, slot])

        def d_begin(name, j):
            own, copy = keep(j)
            copy.start()
            ring(name + "1", j, 0, own)

        def d_turn(name, j):
            arrived(name + "1", j, 1)
            keep(j)[1].wait()
            ring(name + "2", j, 0)

        def d_turn2(name, j):
            arrived(name + "2", j, 1)
            ring("d3", j, 0)

        def either(k, fn):
            at_stage(k, lambda j: pl.when(lax.rem(j, 2) == 0)(lambda: fn("d", j)))
            at_stage(k, lambda j: pl.when(lax.rem(j, 2) == 1)(lambda: fn("e", j)))

        k = nz // 2
        at_stage(4 + k, lambda j: arrived("d3", j, k - 1))
        for i in range(k - 1, 0, -1):
            at_stage(4 + i, lambda j, i=i: ring("d3", j, i))
        either(4, d_turn2)
        either(3, lambda name, j: ring(name + "2", j, 1))
        either(2, d_turn)
        either(1, lambda name, j: ring(name + "1", j, 1))
        either(0, d_begin)
        return carry

    lax.fori_loop(0, total + GATHER_LAG * (nz // 2 + 4), tick, 0)


def gather(ng, nu, nd):
    nx, ny, nz = GRID
    _, rg, ff = ng.shape
    _, rd, d = nd.shape
    f = ff // JOBS
    dma = pltpu.SemaphoreType.DMA
    steps = (nz, ny, nx, nz, nx, ny, nx, ny, nz)
    wide = jax.ShapeDtypeStruct((2, nx, ny, nz * rg, ff), BF)
    og, ou, od = pl.pallas_call(
        functools.partial(gather_kernel, JOBS),
        in_specs=[pl.BlockSpec(memory_space=pltpu.VMEM)] * 3,
        out_specs=[pl.BlockSpec(memory_space=pl.ANY)] * 3,
        out_shape=[wide, wide, jax.ShapeDtypeStruct((2, nx, ny, nz, rd, d), BF)],
        scratch_shapes=[
            pltpu.VMEM((2 * JOBS, nz, rg, f), BF), pltpu.VMEM((2 * JOBS, nz, rg, f), BF),
            pltpu.VMEM((2 * JOBS, nz * rg, f), BF), pltpu.VMEM((2 * JOBS, nz * rg, f), BF),
            dma((3, 2 * JOBS)),
            [(dma((n // 2, 2 * JOBS, 2)), dma((n // 2, 2 * JOBS, 2))) for n in steps],
        ],
        compiler_params=pltpu.CompilerParams(vmem_limit_bytes=GATHER_VMEM, collective_id=1, has_side_effects=True),
        name="gather",
    )(ng, nu, nd)
    n = nx * ny * nz
    return og.reshape(2, n * rg, ff), ou.reshape(2, n * rg, ff), od.reshape(2, n * rd, d)


def adamw(w, m, v, g):
    g = lax.reduce_precision(g, 8, 7)
    m = 0.9 * m + 0.1 * g
    v = 0.95 * v + 0.05 * g * g
    step = m * lax.rsqrt(v + 1e-8) + 0.1 * w
    return (w - 0.02 * step).astype(BF), m, v


def device_step(x, dy, *arrays):
    weights, ms, vs = (arrays[i:i + 3] for i in (0, 3, 6))
    sums = gradients(x[0], dy[0], *weights)
    me = lax.axis_index("dp")
    new = []
    for w, m, v, g in zip(weights, ms, vs, sums, strict=True):
        rows = m.shape[1]
        own = lax.dynamic_slice_in_dim(w, me * rows, rows, 1).astype(F32)
        new.append(adamw(own, m, v, g))
    gathered = gather(*(one[0] for one in new))
    return (*gathered, *(one[1] for one in new), *(one[2] for one in new))


def solution(mesh):
    x, w, m = P(("rep", "dp"), None, None), P(None, None, None), P(None, "dp", None)
    return jax.shard_map(
        device_step,
        mesh=mesh,
        in_specs=(x, x, w, w, w, *[m] * 6),
        out_specs=(*[P("rep", None, None)] * 3, *[P("rep", "dp", None)] * 6),
        check_vma=False,
    )
```

```python
import functools

import jax
import jax.numpy as jnp
from jax import lax
from jax.experimental import pallas as pl
from jax.experimental.pallas import tpu as pltpu
from jax.sharding import PartitionSpec as P

GRID = (4, 4, 8)
BF, F32 = jnp.bfloat16, jnp.float32
MESH = pl.DeviceIdType.MESH
VMEM_LIMIT = 66_000_000
GATHER_VMEM = 12 << 20
LAG = 2
SLOTS = 6
GROUPS = 3
JOBS = 4


def dot(a, b, dims=((1,), (0,))):
    return lax.dot_general(a, b, (dims, ((), ())), preferred_element_type=F32)


def normed(h):
    wide = h.astype(F32)
    scale = lax.rsqrt(jnp.mean(wide**2, -1, keepdims=True) + 1e-6)
    return (wide * scale).astype(BF)


def place():
    nx, ny, nz = GRID
    me = lax.axis_index("dp")
    at = (lax.div(me, ny * nz), lax.rem(lax.div(me, nz), ny), lax.rem(me, nz))

    def neighbour(axis, step):
        c = list(at)
        c[axis] = lax.rem(at[axis] + (step + GRID[axis]), GRID[axis])
        return (c[0] * ny + c[1]) * nz + c[2]

    return at, neighbour


def greet(neighbour, whole):
    steps = [(axis, step) for axis in range(3) for step in (range(1, GRID[axis]) if whole else (1, GRID[axis] - 1))]
    for axis, step in steps:
        pl.semaphore_signal(pltpu.get_barrier_semaphore(), inc=1, device_id={"dp": neighbour(axis, step)}, device_id_type=MESH)
    return len(steps)


class Sender:
    def __init__(self, axis, at, neighbour, send, recv):
        self.n, self.p = GRID[axis], at[axis]
        self.to = (neighbour(axis, 1), neighbour(axis, -1))
        self.send, self.recv = send, recv

    def block(self, step):
        return lax.rem(self.p + (step + self.n), self.n)

    def copy(self, step, slot, d, src, dst):
        return pltpu.make_async_remote_copy(
            src_ref=src, dst_ref=dst, send_sem=self.send.at[step, slot], recv_sem=self.recv.at[step, slot],
            device_id={"dp": self.to[d]}, device_id_type=MESH,
        )

    def wait(self, step, slot, both):
        for sem in (self.recv, self.send):
            pltpu.make_async_copy(both, both, sem.at[step, slot]).wait()


class Direct:
    def __init__(self, axis, at, neighbour, own, stage, recv, send_sem, recv_sem):
        n, p = GRID[axis], at[axis]
        self.own, self.mine = own, p
        self.copies = []
        for q in range(1, n):
            copy = pltpu.make_async_remote_copy(
                src_ref=stage.at[q - 1], dst_ref=recv.at[q - 1], send_sem=send_sem.at[q - 1], recv_sem=recv_sem.at[q - 1],
                device_id={"dp": neighbour(axis, q)}, device_id_type=MESH,
            )
            self.copies.append((lax.rem(p + q, n), stage.at[q - 1], recv.at[q - 1], copy))

    def start(self):
        for block, stage, _, copy in self.copies:
            stage[...] = self.own(block)[...].astype(BF)
            copy.start()

    def finish(self):
        done = self.own(self.mine)[...]
        for _, _, recv, copy in self.copies:
            copy.wait_recv()
            copy.wait_send()
            done = done + recv[...].astype(F32)
        return done


def compute(layer, blocks, a_all, at_all, dh, wg, wu, wd, hid, dgate, dup, da):
    tokens = dgate.shape[0]
    rows = tokens // blocks
    for b in range(blocks):
        s = pl.ds(b * rows, rows)
        a = a_all[layer, s]
        gate = dot(a, wg)
        up = dot(a, wu)
        ct = dot(dh[layer, s], wd, ((1,), (1,))).astype(BF).astype(F32)
        sig = jax.nn.sigmoid(gate)
        silu = gate * sig
        hid[s] = (silu * up).astype(BF)
        dup[s] = (ct * silu).astype(BF)
        dgate[s] = (ct * up * (sig + silu * (1.0 - sig))).astype(BF)

    if layer == 1:
        da[...] += dot(dgate[...], wg, ((1,), (1,))) + dot(dup[...], wu, ((1,), (1,)))

    at = at_all[layer]
    return dot(at, dgate[...]), dot(at, dup[...]), dot(hid[...], dh[layer], ((0,), (0,)))


def reduce_kernel(x, dy, wg, wu, wd, out_g, out_u, out_d, *scratch):
    (hid, dgate, dup, da, dh, a_all, at_all, h1,
     own_g, own_u, own_d, acc_g2, acc_u2, acc_w3, acc_d2, acc_d3,
     rg, ru, rw, rd, sg, su, sw, sd, sems, direct, hold_g, hold_u, hold_d, hold_sem) = scratch
    nx, ny, nz = GRID
    chunks = nx * ny
    total = 2 * chunks
    f = hold_g.shape[2]
    at, neighbour = place()

    senders = {
        name: Sender(axis, at, neighbour, *sem)
        for (name, axis), sem in zip(
            (("g1", 0), ("g2", 1), ("u1", 1), ("u2", 0), ("w3", 2), ("d1", 2), ("d2", 1), ("d3", 0)), sems, strict=True
        )
    }

    def halves(array, ref):
        if array == "w3":
            return ref.at[0], ref.at[1]
        h = ref.shape[0] // 2
        return ref.at[pl.ds(0, h)], ref.at[pl.ds(h, h)]

    def first(array, slot, own, recv):
        s = senders[array]

        def start():
            for d, half in enumerate(halves(array, own(s.block(s.n // 2)))):
                s.copy(0, slot, d, half, recv[0].at[slot, d]).start()

        def middle(j):
            s.wait(j - 1, slot, recv[j - 1].at[slot])
            q = s.n // 2 - j
            for d in (0, 1):
                block = own(s.block(q if d == 0 else -q))
                into = halves(array, block)[d] if j == 1 else block
                into[...] = (into[...].astype(F32) + recv[j - 1][slot, d].astype(F32)).astype(BF)
                s.copy(j, slot, d, block, recv[j].at[slot, d]).start()

        def last():
            j = s.n // 2
            s.wait(j - 1, slot, recv[j - 1].at[slot])
            return own(s.p)[...].astype(F32) + recv[j - 1][slot, 0].astype(F32) + recv[j - 1][slot, 1].astype(F32)

        return start, middle, last

    def later(array, slot, own, recv, stage):
        s = senders[array]

        def start():
            for d, half in enumerate(halves(array, own(s.block(s.n // 2)))):
                stage[0][slot, d] = half[...].astype(BF)
                s.copy(0, slot, d, stage[0].at[slot, d], recv[0].at[slot, d]).start()

        def middle(j):
            s.wait(j - 1, slot, recv[j - 1].at[slot])
            q = s.n // 2 - j
            for d in (0, 1):
                block = own(s.block(q if d == 0 else -q))
                into = halves(array, block)[d] if j == 1 else block
                into[...] = into[...] + recv[j - 1][slot, d].astype(F32)
                stage[j][slot, d] = block[...].astype(BF)
                s.copy(j, slot, d, stage[j].at[slot, d], recv[j].at[slot, d]).start()

        def last():
            j = s.n // 2
            s.wait(j - 1, slot, recv[j - 1].at[slot])
            return own(s.p)[...] + recv[j - 1][slot, 0].astype(F32) + recv[j - 1][slot, 1].astype(F32)

        return start, middle, last

    def layer_of(c):
        return 1 - lax.div(c, chunks)

    def enter(layer, h):
        a = normed(h)
        a_all[layer] = a
        at_all[layer] = a.T

    def begin():
        enter(0, x[...])
        dh[1] = dy[...]
        da[...] = jnp.zeros_like(da)

    def between():
        h = x[...] + da[...].astype(BF)
        h1[...] = h
        enter(1, h)
        da[...] = jnp.zeros_like(da)

    def weights(i, act):
        slot, layer = lax.rem(i, 2), lax.rem(lax.div(i, chunks), 2)
        part = pl.ds(pl.multiple_of(lax.rem(i, chunks) * f, f), f)
        for k, (src, dst) in enumerate(((wg.at[layer, :, part], hold_g), (wu.at[layer, :, part], hold_u), (wd.at[layer, part], hold_d))):
            act(pltpu.make_async_copy(src, dst.at[slot], hold_sem.at[slot, k]))

    def next_weights(i):
        weights(i, lambda c: c.wait())
        pl.when(i + 1 < 3 * chunks)(lambda: weights(i + 1, lambda c: c.start()))
        slot = lax.rem(i, 2)
        return hold_g[slot], hold_u[slot], hold_d[slot]

    def forward(i):
        g, u, d = next_weights(i)
        rows = hid.shape[0] // 2
        for b in range(2):
            s = pl.ds(b * rows, rows)
            gate = dot(a_all[0, s], g)
            up = dot(a_all[0, s], u)
            da[s] += dot((gate * jax.nn.sigmoid(gate) * up).astype(BF), d)

    def exchange(t):
        rings(t, lambda k, every, keep: stage(t, k, every, keep))

    def stage(t, k, every, keep):
        def run(fn):
            c = t - LAG * k
            on = (c >= 0) & (c < total)
            if every > 1:
                on &= lax.rem(c, every) == every - 1
            if keep is not None:
                on &= (c < total - 1) if keep == "early" else (c == total - 1)
            pl.when(on)(functools.partial(fn, c))

        return run

    def rings(t, at_point):
        def at_stage(k, every=1, keep=None):
            return at_point(k, every, keep)

        def d1(c):
            slot, long = lax.rem(c, SLOTS), lax.rem(c, 2 * SLOTS)
            return first("d1", slot, lambda q: own_d.at[long, q], rd[0:4])

        def d2(c):
            slot = lax.rem(lax.div(c, ny), 2)
            return later("d2", slot, lambda q: acc_d2.at[slot, q], rd[4:6], sd[0:2])

        def d3(c):
            slot = layer_of(c)
            return later("d3", slot, lambda q: acc_d3.at[slot, q], rd[6:8], sd[2:4])

        def d2_direct():
            slot = ((total - 1) // ny) % 2
            return Direct(1, at, neighbour, lambda q: acc_d2.at[slot, q], *direct[1])

        def d3_direct():
            return Direct(0, at, neighbour, lambda q: acc_d3.at[0, q], *direct[2])

        def d_last1(c):
            acc_d3[0, nx - 1] = d2_direct().finish()
            d3_direct().start()

        def d_last2(c):
            out_d[0] = d3_direct().finish()

        def d_end(c):
            out_d[layer_of(c)] = d3(c)[2]()

        def d_turn2(c):
            acc_d3[layer_of(c), lax.rem(lax.div(c, ny), nx)] = d2(c)[2]()

        def d_turn1(c):
            acc_d2[lax.rem(lax.div(c, ny), 2), lax.rem(c, ny)] = d1(c)[2]()

        at_stage(8, chunks, "early")(d_end)
        at_stage(7, chunks, "early")(lambda c: d3(c)[1](1))
        at_stage(6, ny, "early")(d_turn2)
        at_stage(6, chunks, "early")(lambda c: d3(c)[0]())
        at_stage(5, ny, "early")(lambda c: d2(c)[1](1))
        at_stage(6, ny, "last")(d_last2)
        at_stage(5, ny, "last")(d_last1)
        at_stage(4)(d_turn1)
        at_stage(4, ny, "early")(lambda c: d2(c)[0]())
        at_stage(4, ny, "last")(lambda c: d2_direct().start())
        for j in (3, 2, 1):
            at_stage(j)(lambda c, j=j: d1(c)[1](j))

        def w3(c):
            slot = lax.rem(lax.div(c, ny), GROUPS)
            return later("w3", slot, lambda q: acc_w3.at[slot, q], rw, sw)

        def w_direct():
            slot = ((total - 1) // ny) % GROUPS
            return Direct(2, at, neighbour, lambda q: acc_w3.at[slot, q], *direct[0])

        def w_end(c, last=False):
            done = w_direct().finish() if last else w3(c)[2]()
            cols = pl.ds(pl.multiple_of(lax.div(lax.rem(c, chunks), ny) * (ny * f), ny * f), ny * f)
            out_g[layer_of(c), :, cols] = done[0]
            out_u[layer_of(c), :, cols] = done[1]

        at_stage(8, ny, "early")(w_end)
        at_stage(5, ny, "last")(lambda c: w_end(c, True))
        for j in (3, 2, 1):
            at_stage(4 + j, ny, "early")(lambda c, j=j: w3(c)[1](j))

        def wide(which, own, acc2, recv, stage):
            def own1(slot):
                return (lambda q: own.at[slot, q]) if which == "g" else (lambda q: own.at[slot, :, q])

            def p1(c):
                slot = lax.rem(c, SLOTS)
                return first(which + "1", slot, own1(slot), recv[0:2])

            def p2(c):
                slot = lax.rem(c, SLOTS)
                return later(which + "2", slot, lambda q: acc2.at[slot, q], recv[2:4], stage[0:2])

            def turn2(c):
                done = p2(c)[2]()
                rows = acc_w3.shape[3]
                cols = pl.ds(pl.multiple_of(lax.rem(c, ny) * f, f), f)
                for q in range(nz):
                    acc_w3[lax.rem(lax.div(c, ny), GROUPS), q, "gu".index(which), :, cols] = done[q * rows:(q + 1) * rows]

            at_stage(4)(turn2)
            at_stage(3)(lambda c: p2(c)[1](1))

            def turn1(c):
                done = p1(c)[2]()
                acc2[lax.rem(c, SLOTS)] = done.reshape(acc2.shape[1:])
                p2(c)[0]()

            at_stage(2)(turn1)
            at_stage(1)(lambda c: p1(c)[1](1))

        wide("g", own_g, acc_g2, rg, sg)
        wide("u", own_u, acc_u2, ru, su)
        at_stage(4, ny, "early")(lambda c: w3(c)[0]())
        at_stage(4, ny, "last")(lambda c: w_direct().start())

    def backward_norm():
        h, by_a = h1[...].astype(F32), da[...].astype(BF).astype(F32)
        scale = lax.rsqrt(jnp.mean(h**2, -1, keepdims=True) + 1e-6)
        by_h = scale * by_a - h * (scale**3 * jnp.mean(by_a * h, -1, keepdims=True))
        dh[0] = dy[...] + by_h.astype(BF)

    def produce(layer, c):
        slot, long = lax.rem(c, SLOTS), lax.rem(c, 2 * SLOTS)
        g, u, d = compute(layer, 4, a_all, at_all, dh, *next_weights(chunks + c), hid, dgate, dup, da)
        own_g[slot] = g.astype(BF).reshape(own_g.shape[1:])
        own_u[slot] = u.astype(BF).reshape(own_u.shape[1:])
        own_d[long] = d.astype(BF).reshape(own_d.shape[1:])
        first("d1", slot, lambda q: own_d.at[long, q], rd[0:4])[0]()
        first("g1", slot, lambda q: own_g.at[slot, q], rg[0:2])[0]()
        first("u1", slot, lambda q: own_u.at[slot, :, q], ru[0:2])[0]()

    def ticks(start, stop, *fns):
        def tick(t, carry):
            for fn in fns:
                fn(t)
            return carry

        lax.fori_loop(start, stop, tick, 0)

    weights(0, lambda c: c.start())
    met = greet(neighbour, True)
    begin()
    ticks(0, chunks, forward)
    pl.semaphore_wait(pltpu.get_barrier_semaphore(), met)
    between()
    ticks(0, chunks, exchange, functools.partial(produce, 1))
    backward_norm()
    ticks(chunks, total, exchange, functools.partial(produce, 0))
    ticks(total, max(total - 1 + 6 * LAG, total - 1 - ny + 8 * LAG) + 1, exchange)


def gradients(x, dy, wg, wu, wd):
    nx, ny, nz = GRID
    n = nx * ny * nz
    tokens, d = x.shape
    ff = wg.shape[2]
    chunks = nx * ny
    f, rg, rd = ff // chunks, d // n, ff // n
    total = 2 * chunks

    s, long = SLOTS, 2 * SLOTS
    g_blocks = [((ny * nz * rg) // 2, f), (ny * nz * rg, f), (nz * rg // 2, f), (nz * rg, f)]
    u_blocks = [(nx // 2, nz * rg, f), (nx, nz * rg, f), (nz * rg // 2, f), (nz * rg, f)]
    w_blocks = [(rg, ny * f)] + [(2, rg, ny * f)] * (nz // 2 - 1)
    d_blocks = [(rd // 2, d)] + [(rd, d)] * (nz // 2 - 1) + [(rd // 2, d), (rd, d)] * 2
    d_slots = [s] * (nz // 2) + [2] * 4
    steps = {"g1": nx, "g2": ny, "u1": ny, "u2": nx, "w3": nz, "d1": nz, "d2": ny, "d3": nx}
    dma = pltpu.SemaphoreType.DMA

    def sems(name, n):
        count = {"d2": 2, "d3": 2, "w3": GROUPS}.get(name, s)
        return (dma((n // 2, count)), dma((n // 2, count)))

    scratch = [
        pltpu.VMEM((tokens, f), BF), pltpu.VMEM((tokens, f), BF), pltpu.VMEM((tokens, f), BF),
        pltpu.VMEM((tokens, d), F32), pltpu.VMEM((2, tokens, d), BF),
        pltpu.VMEM((2, tokens, d), BF), pltpu.VMEM((2, d, tokens), BF), pltpu.VMEM((tokens, d), BF),
        pltpu.VMEM((s, nx, ny * nz * rg, f), BF), pltpu.VMEM((s, nx, ny, nz * rg, f), BF), pltpu.VMEM((long, nz, rd, d), BF),
        pltpu.VMEM((s, ny, nz * rg, f), F32), pltpu.VMEM((s, nx, nz * rg, f), F32),
        pltpu.VMEM((GROUPS, nz, 2, rg, ny * f), F32),
        pltpu.VMEM((2, ny, rd, d), F32), pltpu.VMEM((2, nx, rd, d), F32),
        [pltpu.VMEM((s, 2, *b), BF) for b in g_blocks],
        [pltpu.VMEM((s, 2, *b), BF) for b in u_blocks],
        [pltpu.VMEM((GROUPS, 2, *b), BF) for b in w_blocks],
        [pltpu.VMEM((k, 2, *b), BF) for k, b in zip(d_slots, d_blocks, strict=True)],
        [pltpu.VMEM((s, 2, *b), BF) for b in g_blocks[2:]],
        [pltpu.VMEM((s, 2, *b), BF) for b in u_blocks[2:]],
        [pltpu.VMEM((GROUPS, 2, *b), BF) for b in w_blocks],
        [pltpu.VMEM((k, 2, *b), BF) for k, b in zip(d_slots[nz // 2:], d_blocks[nz // 2:], strict=True)],
        [sems(name, n) for name, n in steps.items()],
        [
            (pltpu.VMEM((n - 1, *b), BF), pltpu.VMEM((n - 1, *b), BF), dma((n - 1,)), dma((n - 1,)))
            for n, b in ((nz, (2, rg, ny * f)), (ny, (rd, d)), (nx, (rd, d)))
        ],
        pltpu.VMEM((2, d, f), BF), pltpu.VMEM((2, d, f), BF), pltpu.VMEM((2, f, d), BF), dma((2, 3)),
    ]
    vmem = pl.BlockSpec(memory_space=pltpu.VMEM)
    return pl.pallas_call(
        reduce_kernel,
        in_specs=[vmem] * 2 + [pl.BlockSpec(memory_space=pl.ANY)] * 3,
        out_specs=[vmem] * 3,
        out_shape=[jax.ShapeDtypeStruct((2, rg, ff), F32)] * 2 + [jax.ShapeDtypeStruct((2, rd, d), F32)],
        scratch_shapes=scratch,
        compiler_params=pltpu.CompilerParams(
            vmem_limit_bytes=VMEM_LIMIT, collective_id=0, has_side_effects=True
        ),
        name="reduce",
    )(x, dy, wg, wu, wd)


def gather_kernel(ng, nu, nd, og, ou, od, *scratch):
    zb, yg, yu, local, sems = scratch
    nx, ny, nz = GRID
    total = 2 * JOBS
    f, r = zb.shape[-1], nd.shape[1] // JOBS
    at, neighbour = place()
    x_, y_, z_ = at
    met = greet(neighbour, False)
    names = (("w1", 2), ("g2", 1), ("g3", 0), ("u2", 0), ("u3", 1), ("d1", 0), ("d2", 1), ("d3", 2))
    odd = (("e1", 1), ("e2", 0), ("e3", 2))
    senders = {name: Sender(axis, at, neighbour, *sem) for (name, axis), sem in zip((*names, *odd), (*sems, *sems[5:]), strict=True)}

    def piece(j):
        return 1 - lax.div(j, JOBS), lax.rem(j, JOBS)

    def blocks(name, j):
        layer, q = piece(j)
        cols, rows = pl.ds(pl.multiple_of(q * f, f), f), pl.ds(pl.multiple_of(q * r, r), r)
        h = nz * ng.shape[1] // 2
        d = nd.shape[2] // 2

        def halves(at_half, n):
            return lambda b: tuple(at_half(b, part) for part in (pl.ds(0, n), pl.ds(n, n)))

        return {
            "w1": (lambda b: zb.at[j, b], lambda b: (zb.at[j, b, 0], zb.at[j, b, 1])),
            "g2": (lambda b: og.at[layer, x_, b, :, cols], halves(lambda b, p: og.at[layer, x_, b, p, cols], h)),
            "u2": (lambda b: ou.at[layer, b, y_, :, cols], halves(lambda b, p: ou.at[layer, b, y_, p, cols], h)),
            "g3": (lambda b: og.at[layer, b, :, :, cols], halves(lambda b, p: og.at[layer, b, p, :, cols], ny // 2)),
            "u3": (lambda b: ou.at[layer, :, b, :, cols], halves(lambda b, p: ou.at[layer, p, b, :, cols], nx // 2)),
            "d1": (lambda b: od.at[layer, b, y_, z_, rows], halves(lambda b, p: od.at[layer, b, y_, z_, rows, p], d)),
            "e1": (lambda b: od.at[layer, x_, b, z_, rows], halves(lambda b, p: od.at[layer, x_, b, z_, rows, p], d)),
            "d2": (lambda b: od.at[layer, :, b, z_, rows], halves(lambda b, p: od.at[layer, p, b, z_, rows], nx // 2)),
            "e2": (lambda b: od.at[layer, b, :, z_, rows], halves(lambda b, p: od.at[layer, b, p, z_, rows], ny // 2)),
            "d3": (lambda b: od.at[layer, :, :, b, rows], halves(lambda b, p: od.at[layer, p, :, b, rows], nx // 2)),
            "e3": (lambda b: od.at[layer, :, :, b, rows], halves(lambda b, p: od.at[layer, p, :, b, rows], nx // 2)),
        }[name]

    def ring(name, j, i, first=None):
        s = senders[name]
        full, half = blocks(name, j)
        if i > 0:
            arrived(name, j, i - 1)
        for d in (0, 1):
            b = s.block(-i if d == 0 else i)
            dst = full(b) if i < s.n // 2 - 1 else half(b)[d]
            s.copy(i, lax.rem(j, SLOTS), d, first if first is not None else dst, dst).start()

    def arrived(name, j, i):
        s = senders[name]
        full = blocks(name, j)[0]
        s.wait(i, lax.rem(j, SLOTS), full(pl.ds(0, 2) if i < s.n // 2 - 1 else 0))

    def tick(t, carry):
        def at_stage(k, fn):
            j = t - LAG * k
            pl.when((j >= 0) & (j < total))(lambda: fn(j))

        def keep(which, j):
            slot = lax.rem(j, SLOTS)
            src, name, b = ((yg, "g2", y_), (yu, "u2", x_))[which]
            return pltpu.make_async_copy(src.at[slot], blocks(name, j)[0](b), local.at[which, slot])

        def begin(j):
            layer, q = piece(j)
            for k, new in enumerate((ng, nu)):
                zb[j, z_, k] = new[layer, :, pl.ds(pl.multiple_of(q * f, f), f)]
            ring("w1", j, 0)

        def turn(j):
            slot = lax.rem(j, SLOTS)
            arrived("w1", j, nz // 2 - 1)
            for which, (yb, name) in enumerate(((yg, "g2"), (yu, "u2"))):
                yb[slot] = zb[j, :, which].reshape(yb.shape[1:])
                keep(which, j).start()
                ring(name, j, 0, yb.at[slot])

        def turn2(j):
            for which, name in enumerate("gu"):
                arrived(name + "2", j, 1)
                keep(which, j).wait()
                ring(name + "3", j, 0)

        def both(fn):
            def run(j):
                for name in "gu":
                    fn(name, j)

            return run

        k = nz // 2
        at_stage(k + 4, both(lambda name, j: arrived(name + "3", j, 1)))
        at_stage(k + 3, both(lambda name, j: ring(name + "3", j, 1)))
        at_stage(k + 2, turn2)
        at_stage(k + 1, both(lambda name, j: ring(name + "2", j, 1)))
        at_stage(k, turn)
        for i in range(k - 1, 0, -1):
            at_stage(i, lambda j, i=i: ring("w1", j, i))
        at_stage(0, begin)

        def own_rows(name, j):
            layer, q = piece(j)
            own = nd.at[layer, pl.ds(pl.multiple_of(q * r, r), r)]
            return own, pltpu.make_async_copy(own, blocks(name + "1", j)[0](x_ if name == "d" else y_), local.at[2, lax.rem(j, SLOTS)])

        def d_begin(name, j):
            own, copy = own_rows(name, j)
            copy.start()
            ring(name + "1", j, 0, own)

        def d_turn(name, j):
            arrived(name + "1", j, 1)
            own_rows(name, j)[1].wait()
            ring(name + "2", j, 0)

        def d_turn2(name, j):
            arrived(name + "2", j, 1)
            ring(name + "3", j, 0)

        def either(k, fn):
            at_stage(k, lambda j: pl.when(lax.rem(j, 2) == 0)(lambda: fn("d", j)))
            at_stage(k, lambda j: pl.when(lax.rem(j, 2) == 1)(lambda: fn("e", j)))

        either(4 + k, lambda name, j: arrived(name + "3", j, k - 1))
        for i in range(k - 1, 0, -1):
            either(4 + i, lambda name, j, i=i: ring(name + "3", j, i))
        either(4, d_turn2)
        either(3, lambda name, j: ring(name + "2", j, 1))
        either(2, d_turn)
        either(1, lambda name, j: ring(name + "1", j, 1))
        either(0, d_begin)
        return carry

    pl.semaphore_wait(pltpu.get_barrier_semaphore(), met)
    lax.fori_loop(0, total + LAG * (nz // 2 + 4), tick, 0)


def gather(ng, nu, nd):
    nx, ny, nz = GRID
    _, rg, ff = ng.shape
    _, rd, d = nd.shape
    f, jobs = ff // JOBS, 2 * JOBS
    dma = pltpu.SemaphoreType.DMA
    steps = (nz, ny, nx, nx, ny, nx, ny, nz)
    wide = jax.ShapeDtypeStruct((2, nx, ny, nz * rg, ff), BF)
    got = pl.pallas_call(
        gather_kernel,
        in_specs=[pl.BlockSpec(memory_space=pltpu.VMEM)] * 3,
        out_specs=[pl.BlockSpec(memory_space=pl.ANY)] * 3,
        out_shape=[wide, wide, jax.ShapeDtypeStruct((2, nx, ny, nz, rd, d), BF)],
        scratch_shapes=[
            pltpu.VMEM((jobs, nz, 2, rg, f), BF), pltpu.VMEM((SLOTS, nz * rg, f), BF), pltpu.VMEM((SLOTS, nz * rg, f), BF),
            dma((3, SLOTS)),
            [(dma((n // 2, SLOTS)), dma((n // 2, SLOTS))) for n in steps],
        ],
        compiler_params=pltpu.CompilerParams(vmem_limit_bytes=GATHER_VMEM, collective_id=1, has_side_effects=True),
        name="gather",
    )(ng, nu, nd)
    og, ou, od = emit(*got)
    n = nx * ny * nz
    return og.reshape(2, n * rg, ff), ou.reshape(2, n * rg, ff), od.reshape(2, n * rd, d)


def emit_kernel(g, u, d, go, uo, do, hold, sems):
    copies = [pltpu.make_async_copy(a.at[i], b.at[i], sems.at[k, i]) for k, (a, b) in enumerate(((g, go), (u, uo))) for i in range(2)]
    for c in copies:
        c.start()
    pieces = [(i, x) for i in range(2) for x in range(4)]
    slots = hold.shape[0]
    ins = [pltpu.make_async_copy(d.at[p], hold.at[k % slots], sems.at[2, k]) for k, p in enumerate(pieces)]
    outs = [pltpu.make_async_copy(hold.at[k % slots], do.at[p], sems.at[3, k]) for k, p in enumerate(pieces)]
    for c in ins[:slots]:
        c.start()
    for k in range(len(pieces)):
        ins[k].wait()
        outs[k].start()
        if k >= 1 and k - 1 + slots < len(pieces):
            outs[k - 1].wait()
            ins[k - 1 + slots].start()
    for c in outs[len(pieces) - slots:] + copies:
        c.wait()


def emit(*arrays):
    return pl.pallas_call(
        emit_kernel,
        in_specs=[pl.BlockSpec(memory_space=pltpu.VMEM), pl.BlockSpec(memory_space=pltpu.VMEM), pl.BlockSpec(memory_space=pltpu.HBM)],
        out_specs=[pl.BlockSpec(memory_space=pltpu.HBM)] * 3,
        out_shape=[jax.ShapeDtypeStruct(a.shape, BF) for a in arrays],
        scratch_shapes=[pltpu.VMEM((3, *arrays[2].shape[2:]), BF), pltpu.SemaphoreType.DMA((4, 8))],
        compiler_params=pltpu.CompilerParams(vmem_limit_bytes=7 << 20),
        name="emit",
    )(*arrays)


def adamw(w, m, v, g):
    g = lax.reduce_precision(g, 8, 7)
    m = 0.9 * m + 0.1 * g
    v = 0.95 * v + 0.05 * g * g
    step = m * lax.rsqrt(v + 1e-8) + 0.1 * w
    return (w - 0.02 * step).astype(BF), m, v


def device_step(x, dy, *arrays):
    weights, ms, vs = (arrays[i:i + 3] for i in (0, 3, 6))
    sums = gradients(x[0], dy[0], *weights)
    me = lax.axis_index("dp")
    new = []
    for w, m, v, g in zip(weights, ms, vs, sums, strict=True):
        rows = m.shape[1]
        own = lax.dynamic_slice_in_dim(w, me * rows, rows, 1).astype(F32)
        new.append(adamw(own, m, v, g))
    gathered = gather(*(one[0] for one in new))
    return (*gathered, *(one[1] for one in new), *(one[2] for one in new))


def solution(mesh):
    x, w, m = P(("rep", "dp"), None, None), P(None, None, None), P(None, "dp", None)
    return jax.shard_map(
        device_step,
        mesh=mesh,
        in_specs=(x, x, w, w, w, *[m] * 6),
        out_specs=(*[P("rep", None, None)] * 3, *[P("rep", "dp", None)] * 6),
        check_vma=False,
    )
```

```python
import functools

import jax
import jax.numpy as jnp
from jax import lax
from jax.experimental import pallas as pl
from jax.experimental.pallas import tpu as pltpu
from jax.sharding import PartitionSpec as P

GRID = (4, 4, 8)
BF, F32 = jnp.bfloat16, jnp.float32
ALL = Ellipsis
MESH = pl.DeviceIdType.MESH
VMEM_LIMIT = 66_000_000
GATHER_LAG = 3
EMIT_VMEM = 10 << 20
GATHER_VMEM = 12 << 20
LAG = 2
SLOTS = 6
GROUPS = 3
JOBS = 4


def dot(a, b, dims=((1,), (0,))):
    return lax.dot_general(a, b, (dims, ((), ())), preferred_element_type=F32)


def normed(h):
    wide = h.astype(F32)
    scale = lax.rsqrt(jnp.mean(wide**2, -1, keepdims=True) + 1e-6)
    return (wide * scale).astype(BF)


def place():
    nx, ny, nz = GRID
    me = lax.axis_index("dp")
    at = (lax.div(me, ny * nz), lax.rem(lax.div(me, nz), ny), lax.rem(me, nz))

    def neighbour(axis, step):
        c = list(at)
        c[axis] = lax.rem(at[axis] + (step + GRID[axis]), GRID[axis])
        return (c[0] * ny + c[1]) * nz + c[2]

    return at, neighbour


def greet(neighbour, whole):
    steps = [(axis, step) for axis in range(3) for step in (range(1, GRID[axis]) if whole else (1, GRID[axis] - 1))]
    for axis, step in steps:
        pl.semaphore_signal(pltpu.get_barrier_semaphore(), inc=1, device_id={"dp": neighbour(axis, step)}, device_id_type=MESH)
    return len(steps)


class Sender:
    def __init__(self, axis, at, neighbour, send, recv):
        self.n, self.p = GRID[axis], at[axis]
        self.to = (neighbour(axis, 1), neighbour(axis, -1))
        self.send, self.recv = send, recv
        self.slots = bool(send.shape)

    def block(self, step):
        return lax.rem(self.p + (step + self.n), self.n)

    def copy(self, step, slot, d, src, dst):
        return pltpu.make_async_remote_copy(
            src_ref=src, dst_ref=dst, send_sem=self.send.at[step, slot] if self.slots else self.send, recv_sem=self.recv.at[step, slot],
            device_id={"dp": self.to[d]}, device_id_type=MESH,
        )

    def wait(self, step, slot, both):
        for sem in (self.recv, self.send) if self.slots else (self.recv,):
            pltpu.make_async_copy(both, both, sem.at[step, slot]).wait()


class Direct:
    def __init__(self, axis, at, neighbour, own, stage, recv, send_sem, recv_sem):
        n, p = GRID[axis], at[axis]
        self.own, self.mine = own, p
        self.copies = []
        for q in range(1, n):
            copy = pltpu.make_async_remote_copy(
                src_ref=stage.at[q - 1], dst_ref=recv.at[q - 1], send_sem=send_sem.at[q - 1], recv_sem=recv_sem.at[q - 1],
                device_id={"dp": neighbour(axis, q)}, device_id_type=MESH,
            )
            self.copies.append((lax.rem(p + q, n), stage.at[q - 1], recv.at[q - 1], copy))

    def start(self):
        for block, stage, _, copy in self.copies:
            stage[ALL] = self.own(block)[ALL].astype(BF)
            copy.start()

    def finish(self):
        done = self.own(self.mine)[ALL]
        for _, _, recv, copy in self.copies:
            copy.wait_recv()
            copy.wait_send()
            done = done + recv[ALL].astype(F32)
        return done


def compute(layer, blocks, a_all, at_all, dh, wg, wu, wd, hid, dgate, dup, da):
    tokens = dgate.shape[0]
    rows = tokens // blocks
    for b in range(blocks):
        s = pl.ds(b * rows, rows)
        a = a_all[layer, s]
        gate = dot(a, wg)
        up = dot(a, wu)
        ct = dot(dh[layer, s], wd, ((1,), (1,))).astype(BF).astype(F32)
        sig = jax.nn.sigmoid(gate)
        silu = gate * sig
        hid[s] = (silu * up).astype(BF)
        dup[s] = (ct * silu).astype(BF)
        dgate[s] = (ct * up * (sig + silu * (1.0 - sig))).astype(BF)

    if layer == 1:
        da[ALL] += dot(dgate[ALL], wg, ((1,), (1,))) + dot(dup[ALL], wu, ((1,), (1,)))

    at = at_all[layer]
    return dot(at, dgate[ALL]), dot(at, dup[ALL]), dot(hid[ALL], dh[layer], ((0,), (0,)))


def reduce_kernel(x, dy, wg, wu, wd, out_g, out_u, out_d, *scratch):
    (hid, dgate, dup, da, dh, a_all, at_all, h1,
     own_g, own_u, own_d, acc_g2, acc_u2, acc_w3, acc_d2, acc_d3,
     rg, ru, rw, rd, sg, su, sw, sd, sems, direct, hold_g, hold_u, hold_d, hold_sem) = scratch
    nx, ny, nz = GRID
    chunks = nx * ny
    total = 2 * chunks
    f = hold_g.shape[2]
    at, neighbour = place()

    senders = {
        name: Sender(axis, at, neighbour, *sem)
        for (name, axis), sem in zip(
            (("g1", 0), ("g2", 1), ("u1", 1), ("u2", 0), ("w3", 2), ("d1", 2), ("d2", 1), ("d3", 0)), sems, strict=True
        )
    }

    def halves(array, ref):
        if array == "w3":
            return ref.at[0], ref.at[1]
        h = ref.shape[0] // 2
        return ref.at[pl.ds(0, h)], ref.at[pl.ds(h, h)]

    def first(array, slot, own, recv):
        s = senders[array]

        def start():
            for d, half in enumerate(halves(array, own(s.block(s.n // 2)))):
                s.copy(0, slot, d, half, recv[0].at[slot, d]).start()

        def middle(j):
            s.wait(j - 1, slot, recv[j - 1].at[slot])
            q = s.n // 2 - j
            for d in (0, 1):
                block = own(s.block(q if d == 0 else -q))
                into = halves(array, block)[d] if j == 1 else block
                into[ALL] = (into[ALL].astype(F32) + recv[j - 1][slot, d].astype(F32)).astype(BF)
                s.copy(j, slot, d, block, recv[j].at[slot, d]).start()

        def last():
            j = s.n // 2
            s.wait(j - 1, slot, recv[j - 1].at[slot])
            return own(s.p)[ALL].astype(F32) + recv[j - 1][slot, 0].astype(F32) + recv[j - 1][slot, 1].astype(F32)

        return start, middle, last

    def later(array, slot, own, recv, stage):
        s = senders[array]

        def start():
            for d, half in enumerate(halves(array, own(s.block(s.n // 2)))):
                stage[0][slot, d] = half[ALL].astype(BF)
                s.copy(0, slot, d, stage[0].at[slot, d], recv[0].at[slot, d]).start()

        def middle(j):
            s.wait(j - 1, slot, recv[j - 1].at[slot])
            q = s.n // 2 - j
            for d in (0, 1):
                block = own(s.block(q if d == 0 else -q))
                into = halves(array, block)[d] if j == 1 else block
                into[ALL] = into[ALL] + recv[j - 1][slot, d].astype(F32)
                stage[j][slot, d] = block[ALL].astype(BF)
                s.copy(j, slot, d, stage[j].at[slot, d], recv[j].at[slot, d]).start()

        def last():
            j = s.n // 2
            s.wait(j - 1, slot, recv[j - 1].at[slot])
            return own(s.p)[ALL] + recv[j - 1][slot, 0].astype(F32) + recv[j - 1][slot, 1].astype(F32)

        return start, middle, last

    def layer_of(c):
        return 1 - lax.div(c, chunks)

    def enter(layer, h):
        a = normed(h)
        a_all[layer] = a
        at_all[layer] = a.T

    def begin():
        enter(0, x[ALL])
        dh[1] = dy[ALL]
        da[ALL] = jnp.zeros_like(da)

    def between():
        h = x[ALL] + da[ALL].astype(BF)
        h1[ALL] = h
        enter(1, h)
        da[ALL] = jnp.zeros_like(da)

    def weights(i, act):
        slot, layer = lax.rem(i, 2), lax.rem(lax.div(i, chunks), 2)
        part = pl.ds(pl.multiple_of(lax.rem(i, chunks) * f, f), f)
        for k, (src, dst) in enumerate(((wg.at[layer, :, part], hold_g), (wu.at[layer, :, part], hold_u), (wd.at[layer, part], hold_d))):
            act(pltpu.make_async_copy(src, dst.at[slot], hold_sem.at[slot, k]))

    def next_weights(i):
        weights(i, lambda c: c.wait())
        pl.when(i + 1 < 3 * chunks)(lambda: weights(i + 1, lambda c: c.start()))
        slot = lax.rem(i, 2)
        return hold_g[slot], hold_u[slot], hold_d[slot]

    def forward(i):
        g, u, d = next_weights(i)
        rows = hid.shape[0] // 2
        for b in range(2):
            s = pl.ds(b * rows, rows)
            gate = dot(a_all[0, s], g)
            up = dot(a_all[0, s], u)
            da[s] += dot((gate * jax.nn.sigmoid(gate) * up).astype(BF), d)

    def exchange(t):
        rings(t, lambda k, every, keep: stage(t, k, every, keep))

    def stage(t, k, every, keep):
        def run(fn):
            c = t - LAG * k
            on = (c >= 0) & (c < total)
            if every > 1:
                on &= lax.rem(c, every) == every - 1
            if keep is not None:
                on &= (c < total - 1) if keep == "early" else (c == total - 1)
            pl.when(on)(functools.partial(fn, c))

        return run

    def rings(t, at_point):
        def at_stage(k, every=1, keep=None):
            return at_point(k, every, keep)

        def d1(c):
            slot, long = lax.rem(c, SLOTS), lax.rem(c, 2 * SLOTS)
            return first("d1", slot, lambda q: own_d.at[long, q], rd[0:4])

        def d2(c):
            slot = lax.rem(lax.div(c, ny), 2)
            return later("d2", slot, lambda q: acc_d2.at[slot, q], rd[4:6], sd[0:2])

        def d3(c):
            slot = layer_of(c)
            return later("d3", slot, lambda q: acc_d3.at[slot, q], rd[6:8], sd[2:4])

        def d2_direct():
            slot = ((total - 1) // ny) % 2
            return Direct(1, at, neighbour, lambda q: acc_d2.at[slot, q], *direct[1])

        def d3_direct():
            return Direct(0, at, neighbour, lambda q: acc_d3.at[0, q], *direct[2])

        def d_last1(c):
            acc_d3[0, nx - 1] = d2_direct().finish()
            d3_direct().start()

        def d_last2(c):
            out_d[0] = d3_direct().finish()

        def d_end(c):
            out_d[layer_of(c)] = d3(c)[2]()

        def d_turn2(c):
            acc_d3[layer_of(c), lax.rem(lax.div(c, ny), nx)] = d2(c)[2]()

        def d_turn1(c):
            acc_d2[lax.rem(lax.div(c, ny), 2), lax.rem(c, ny)] = d1(c)[2]()

        at_stage(8, chunks, "early")(d_end)
        at_stage(7, chunks, "early")(lambda c: d3(c)[1](1))
        at_stage(6, ny, "early")(d_turn2)
        at_stage(6, chunks, "early")(lambda c: d3(c)[0]())
        at_stage(5, ny, "early")(lambda c: d2(c)[1](1))
        at_stage(6, ny, "last")(d_last2)
        at_stage(5, ny, "last")(d_last1)
        at_stage(4)(d_turn1)
        at_stage(4, ny, "early")(lambda c: d2(c)[0]())
        at_stage(4, ny, "last")(lambda c: d2_direct().start())
        for j in (3, 2, 1):
            at_stage(j)(lambda c, j=j: d1(c)[1](j))

        def w3(c):
            slot = lax.rem(lax.div(c, ny), GROUPS)
            return later("w3", slot, lambda q: acc_w3.at[slot, q], rw, sw)

        def w_direct():
            slot = ((total - 1) // ny) % GROUPS
            return Direct(2, at, neighbour, lambda q: acc_w3.at[slot, q], *direct[0])

        def w_end(c, last=False):
            done = w_direct().finish() if last else w3(c)[2]()
            cols = pl.ds(pl.multiple_of(lax.div(lax.rem(c, chunks), ny) * (ny * f), ny * f), ny * f)
            out_g[layer_of(c), :, cols] = done[0]
            out_u[layer_of(c), :, cols] = done[1]

        at_stage(8, ny, "early")(w_end)
        at_stage(5, ny, "last")(lambda c: w_end(c, True))
        for j in (3, 2, 1):
            at_stage(4 + j, ny, "early")(lambda c, j=j: w3(c)[1](j))

        def wide(which, own, acc2, recv, stage):
            def own1(slot):
                return (lambda q: own.at[slot, q]) if which == "g" else (lambda q: own.at[slot, :, q])

            def p1(c):
                slot = lax.rem(c, SLOTS)
                return first(which + "1", slot, own1(slot), recv[0:2])

            def p2(c):
                slot = lax.rem(c, SLOTS)
                return later(which + "2", slot, lambda q: acc2.at[slot, q], recv[2:4], stage[0:2])

            def turn2(c):
                done = p2(c)[2]()
                rows = acc_w3.shape[3]
                cols = pl.ds(pl.multiple_of(lax.rem(c, ny) * f, f), f)
                for q in range(nz):
                    acc_w3[lax.rem(lax.div(c, ny), GROUPS), q, "gu".index(which), :, cols] = done[q * rows:(q + 1) * rows]

            at_stage(4)(turn2)
            at_stage(3)(lambda c: p2(c)[1](1))

            def turn1(c):
                done = p1(c)[2]()
                acc2[lax.rem(c, SLOTS)] = done.reshape(acc2.shape[1:])
                p2(c)[0]()

            at_stage(2)(turn1)
            at_stage(1)(lambda c: p1(c)[1](1))

        wide("g", own_g, acc_g2, rg, sg)
        wide("u", own_u, acc_u2, ru, su)
        at_stage(4, ny, "early")(lambda c: w3(c)[0]())
        at_stage(4, ny, "last")(lambda c: w_direct().start())

    def backward_norm():
        h, by_a = h1[ALL].astype(F32), da[ALL].astype(BF).astype(F32)
        scale = lax.rsqrt(jnp.mean(h**2, -1, keepdims=True) + 1e-6)
        by_h = scale * by_a - h * (scale**3 * jnp.mean(by_a * h, -1, keepdims=True))
        dh[0] = dy[ALL] + by_h.astype(BF)

    def produce(layer, c):
        slot, long = lax.rem(c, SLOTS), lax.rem(c, 2 * SLOTS)
        g, u, d = compute(layer, 4, a_all, at_all, dh, *next_weights(chunks + c), hid, dgate, dup, da)
        own_g[slot] = g.astype(BF).reshape(own_g.shape[1:])
        own_u[slot] = u.astype(BF).reshape(own_u.shape[1:])
        own_d[long] = d.astype(BF).reshape(own_d.shape[1:])
        first("d1", slot, lambda q: own_d.at[long, q], rd[0:4])[0]()
        first("g1", slot, lambda q: own_g.at[slot, q], rg[0:2])[0]()
        first("u1", slot, lambda q: own_u.at[slot, :, q], ru[0:2])[0]()

    def ticks(start, stop, *fns):
        def tick(t, carry):
            for fn in fns:
                fn(t)
            return carry

        lax.fori_loop(start, stop, tick, 0)

    weights(0, lambda c: c.start())
    met = greet(neighbour, True)
    begin()
    ticks(0, chunks, forward)
    pl.semaphore_wait(pltpu.get_barrier_semaphore(), met)
    between()
    ticks(0, chunks, exchange, functools.partial(produce, 1))
    backward_norm()
    ticks(chunks, total, exchange, functools.partial(produce, 0))
    ticks(total, max(total - 1 + 6 * LAG, total - 1 - ny + 8 * LAG) + 1, exchange)


def gradients(x, dy, wg, wu, wd):
    nx, ny, nz = GRID
    n = nx * ny * nz
    tokens, d = x.shape
    ff = wg.shape[2]
    chunks = nx * ny
    f, rg, rd = ff // chunks, d // n, ff // n
    total = 2 * chunks

    s, long = SLOTS, 2 * SLOTS
    g_blocks = [((ny * nz * rg) // 2, f), (ny * nz * rg, f), (nz * rg // 2, f), (nz * rg, f)]
    u_blocks = [(nx // 2, nz * rg, f), (nx, nz * rg, f), (nz * rg // 2, f), (nz * rg, f)]
    w_blocks = [(rg, ny * f)] + [(2, rg, ny * f)] * (nz // 2 - 1)
    d_blocks = [(rd // 2, d)] + [(rd, d)] * (nz // 2 - 1) + [(rd // 2, d), (rd, d)] * 2
    d_slots = [s] * (nz // 2) + [2] * 4
    steps = {"g1": nx, "g2": ny, "u1": ny, "u2": nx, "w3": nz, "d1": nz, "d2": ny, "d3": nx}
    dma = pltpu.SemaphoreType.DMA

    def sems(name, n):
        count = {"d2": 2, "d3": 2, "w3": GROUPS}.get(name, s)
        return (dma((n // 2, count)), dma((n // 2, count)))

    scratch = [
        pltpu.VMEM((tokens, f), BF), pltpu.VMEM((tokens, f), BF), pltpu.VMEM((tokens, f), BF),
        pltpu.VMEM((tokens, d), F32), pltpu.VMEM((2, tokens, d), BF),
        pltpu.VMEM((2, tokens, d), BF), pltpu.VMEM((2, d, tokens), BF), pltpu.VMEM((tokens, d), BF),
        pltpu.VMEM((s, nx, ny * nz * rg, f), BF), pltpu.VMEM((s, nx, ny, nz * rg, f), BF), pltpu.VMEM((long, nz, rd, d), BF),
        pltpu.VMEM((s, ny, nz * rg, f), F32), pltpu.VMEM((s, nx, nz * rg, f), F32),
        pltpu.VMEM((GROUPS, nz, 2, rg, ny * f), F32),
        pltpu.VMEM((2, ny, rd, d), F32), pltpu.VMEM((2, nx, rd, d), F32),
        [pltpu.VMEM((s, 2, *b), BF) for b in g_blocks],
        [pltpu.VMEM((s, 2, *b), BF) for b in u_blocks],
        [pltpu.VMEM((GROUPS, 2, *b), BF) for b in w_blocks],
        [pltpu.VMEM((k, 2, *b), BF) for k, b in zip(d_slots, d_blocks, strict=True)],
        [pltpu.VMEM((s, 2, *b), BF) for b in g_blocks[2:]],
        [pltpu.VMEM((s, 2, *b), BF) for b in u_blocks[2:]],
        [pltpu.VMEM((GROUPS, 2, *b), BF) for b in w_blocks],
        [pltpu.VMEM((k, 2, *b), BF) for k, b in zip(d_slots[nz // 2:], d_blocks[nz // 2:], strict=True)],
        [sems(name, n) for name, n in steps.items()],
        [
            (pltpu.VMEM((n - 1, *b), BF), pltpu.VMEM((n - 1, *b), BF), dma((n - 1,)), dma((n - 1,)))
            for n, b in ((nz, (2, rg, ny * f)), (ny, (rd, d)), (nx, (rd, d)))
        ],
        pltpu.VMEM((2, d, f), BF), pltpu.VMEM((2, d, f), BF), pltpu.VMEM((2, f, d), BF), dma((2, 3)),
    ]
    vmem = pl.BlockSpec(memory_space=pltpu.VMEM)
    return pl.pallas_call(
        reduce_kernel,
        in_specs=[vmem] * 2 + [pl.BlockSpec(memory_space=pl.ANY)] * 3,
        out_specs=[vmem] * 3,
        out_shape=[jax.ShapeDtypeStruct((2, rg, ff), F32)] * 2 + [jax.ShapeDtypeStruct((2, rd, d), F32)],
        scratch_shapes=scratch,
        compiler_params=pltpu.CompilerParams(
            vmem_limit_bytes=VMEM_LIMIT, collective_id=0, has_side_effects=True
        ),
        name="reduce",
    )(x, dy, wg, wu, wd)


def gather_kernel(sums, m, v, weights, og, ou, od, *scratch):
    ng, nu, nd, rows_gu, rows_d, sums_held, m_held, v_held, zb, yg, yu, local, rows_sem, held_sem, sems = scratch
    nx, ny, nz = GRID
    total = 2 * JOBS
    f, r = zb.shape[-1], nd.shape[1] // JOBS
    at, neighbour = place()
    x_, y_, z_ = at
    met = greet(neighbour, False)
    me = lax.axis_index("dp")
    rg, rd = ng.shape[1], nd.shape[1]
    eight = pl.ds(pl.multiple_of(lax.div(me, 8 // rg) * 8, 8), 8)
    own = [pltpu.make_async_copy(w.at[:, eight], rows_gu.at[k], rows_sem.at[k]) for k, w in enumerate(weights[:2])]
    own.append(pltpu.make_async_copy(weights[2].at[:, pl.ds(pl.multiple_of(me * rd, rd), rd)], rows_d, rows_sem.at[2]))
    for i, (a, b) in enumerate(((sums, sums_held), (m, m_held), (v, v_held))):
        own += [pltpu.make_async_copy(a[k], b[k], held_sem.at[i, k]) for k in range(3)]
    for c in own:
        c.start()
    for c in own:
        c.wait()
    upper = lax.rem(me, 8 // rg) == 1
    for k, new in enumerate((ng, nu)):
        w = jnp.where(upper, rows_gu[k, :, rg:].astype(F32), rows_gu[k, :, :rg].astype(F32))
        new[ALL] = adamw(w, m_held[k][ALL], v_held[k][ALL], sums_held[k][ALL])[0]
    nd[ALL] = adamw(rows_d[ALL].astype(F32), m_held[2][ALL], v_held[2][ALL], sums_held[2][ALL])[0]
    names = (("w1", 2), ("g2", 1), ("g3", 0), ("u2", 0), ("u3", 1), ("d1", 0), ("d2", 1), ("d3", 2))
    odd = (("e1", 1), ("e2", 0), ("e3", 2))
    senders = {name: Sender(axis, at, neighbour, *sem) for (name, axis), sem in zip((*names, *odd), (*sems, *sems[5:]), strict=True)}

    def piece(j):
        return 1 - lax.div(j, JOBS), lax.rem(j, JOBS)

    def blocks(name, j):
        layer, q = piece(j)
        cols, rows = pl.ds(pl.multiple_of(q * f, f), f), pl.ds(pl.multiple_of(q * r, r), r)
        h = nz * ng.shape[1] // 2
        d = nd.shape[2] // 2

        def halves(at_half, n):
            return lambda b: tuple(at_half(b, part) for part in (pl.ds(0, n), pl.ds(n, n)))

        return {
            "w1": (lambda b: zb.at[j, b], lambda b: (zb.at[j, b, 0], zb.at[j, b, 1])),
            "g2": (lambda b: og.at[layer, x_, b, :, cols], halves(lambda b, p: og.at[layer, x_, b, p, cols], h)),
            "u2": (lambda b: ou.at[layer, b, y_, :, cols], halves(lambda b, p: ou.at[layer, b, y_, p, cols], h)),
            "g3": (lambda b: og.at[layer, b, :, :, cols], halves(lambda b, p: og.at[layer, b, p, :, cols], ny // 2)),
            "u3": (lambda b: ou.at[layer, :, b, :, cols], halves(lambda b, p: ou.at[layer, p, b, :, cols], nx // 2)),
            "d1": (lambda b: od.at[layer, b, y_, z_, rows], halves(lambda b, p: od.at[layer, b, y_, z_, rows, p], d)),
            "e1": (lambda b: od.at[layer, x_, b, z_, rows], halves(lambda b, p: od.at[layer, x_, b, z_, rows, p], d)),
            "d2": (lambda b: od.at[layer, :, b, z_, rows], halves(lambda b, p: od.at[layer, p, b, z_, rows], nx // 2)),
            "e2": (lambda b: od.at[layer, b, :, z_, rows], halves(lambda b, p: od.at[layer, b, p, z_, rows], ny // 2)),
            "d3": (lambda b: od.at[layer, :, :, b, rows], halves(lambda b, p: od.at[layer, p, :, b, rows], nx // 2)),
            "e3": (lambda b: od.at[layer, :, :, b, rows], halves(lambda b, p: od.at[layer, p, :, b, rows], nx // 2)),
        }[name]

    def ring(name, j, i, first=None):
        s = senders[name]
        full, half = blocks(name, j)
        if i > 0:
            arrived(name, j, i - 1)
        for d in (0, 1):
            b = s.block(-i if d == 0 else i)
            dst = full(b) if i < s.n // 2 - 1 else half(b)[d]
            s.copy(i, j, d, first if first is not None else dst, dst).start()

    def arrived(name, j, i):
        s = senders[name]
        full = blocks(name, j)[0]
        s.wait(i, j, full(pl.ds(0, 2) if i < s.n // 2 - 1 else 0))

    def tick(t, carry):
        def at_stage(k, fn):
            j = t - GATHER_LAG * k
            pl.when((j >= 0) & (j < total))(lambda: fn(j))

        def keep(which, j):
            slot = j
            src, name, b = ((yg, "g2", y_), (yu, "u2", x_))[which]
            return pltpu.make_async_copy(src.at[slot], blocks(name, j)[0](b), local.at[which, slot])

        def begin(j):
            layer, q = piece(j)
            for k, new in enumerate((ng, nu)):
                zb[j, z_, k] = new[layer, :, pl.ds(pl.multiple_of(q * f, f), f)]
            ring("w1", j, 0)

        def turn(j):
            slot = j
            arrived("w1", j, nz // 2 - 1)
            for which, (yb, name) in enumerate(((yg, "g2"), (yu, "u2"))):
                yb[slot] = zb[j, :, which].reshape(yb.shape[1:])
                keep(which, j).start()
                ring(name, j, 0, yb.at[slot])

        def turn2(j):
            for which, name in enumerate("gu"):
                arrived(name + "2", j, 1)
                keep(which, j).wait()
                ring(name + "3", j, 0)

        def both(fn):
            def run(j):
                for name in "gu":
                    fn(name, j)

            return run

        k = nz // 2
        at_stage(k + 4, both(lambda name, j: arrived(name + "3", j, 1)))
        at_stage(k + 3, both(lambda name, j: ring(name + "3", j, 1)))
        at_stage(k + 2, turn2)
        at_stage(k + 1, both(lambda name, j: ring(name + "2", j, 1)))
        at_stage(k, turn)
        for i in range(k - 1, 0, -1):
            at_stage(i, lambda j, i=i: ring("w1", j, i))
        at_stage(0, begin)

        def own_rows(name, j):
            layer, q = piece(j)
            own = nd.at[layer, pl.ds(pl.multiple_of(q * r, r), r)]
            return own, pltpu.make_async_copy(own, blocks(name + "1", j)[0](x_ if name == "d" else y_), local.at[2, j])

        def d_begin(name, j):
            own, copy = own_rows(name, j)
            copy.start()
            ring(name + "1", j, 0, own)

        def d_turn(name, j):
            arrived(name + "1", j, 1)
            own_rows(name, j)[1].wait()
            ring(name + "2", j, 0)

        def d_turn2(name, j):
            arrived(name + "2", j, 1)
            ring(name + "3", j, 0)

        def either(k, fn):
            at_stage(k, lambda j: pl.when(lax.rem(j, 2) == 0)(lambda: fn("d", j)))
            at_stage(k, lambda j: pl.when(lax.rem(j, 2) == 1)(lambda: fn("e", j)))

        either(4 + k, lambda name, j: arrived(name + "3", j, k - 1))
        for i in range(k - 1, 0, -1):
            either(4 + i, lambda name, j, i=i: ring(name + "3", j, i))
        either(4, d_turn2)
        either(3, lambda name, j: ring(name + "2", j, 1))
        either(2, d_turn)
        either(1, lambda name, j: ring(name + "1", j, 1))
        either(0, d_begin)
        return carry

    pl.semaphore_wait(pltpu.get_barrier_semaphore(), met)
    lax.fori_loop(0, total + GATHER_LAG * (nz // 2 + 4), tick, 0)
    xs, ys, zs = (pl.ds(0, n - 1) for n in GRID)
    sent = (zb.at[:, zs], og.at[:, xs, 0], og.at[:, xs], ou.at[:, ys, 0], ou.at[:, :, ys], od.at[:, xs, 0, 0], od.at[:, :, ys, 0], od.at[:, :, :, zs])
    for (send, _), what in zip(sems, sent, strict=True):
        pltpu.make_async_copy(what, what, send).wait()


def gather(sums, m, v, weights):
    nx, ny, nz = GRID
    _, rg, ff = sums[0].shape
    _, rd, d = sums[2].shape
    hbm = [pl.BlockSpec(memory_space=pltpu.HBM)] * 3
    held = [pltpu.VMEM(a.shape, F32) for a in m]
    f, jobs = ff // JOBS, 2 * JOBS
    dma = pltpu.SemaphoreType.DMA
    steps = (nz, ny, nx, nx, ny, nx, ny, nz)
    wide = jax.ShapeDtypeStruct((2, nx, ny, nz * rg, ff), BF)
    return pl.pallas_call(
        gather_kernel,
        in_specs=[hbm] * 4,
        out_specs=[pl.BlockSpec(memory_space=pl.ANY)] * 3,
        out_shape=[wide, wide, jax.ShapeDtypeStruct((2, nx, ny, nz, rd, d), BF)],
        scratch_shapes=[
            pltpu.VMEM((2, rg, ff), BF), pltpu.VMEM((2, rg, ff), BF), pltpu.VMEM((2, rd, d), BF),
            pltpu.VMEM((2, 2, 8, ff), BF), pltpu.VMEM((2, rd, d), BF), held, held, held,
            pltpu.VMEM((jobs, nz, 2, rg, f), BF), pltpu.VMEM((jobs, nz * rg, f), BF), pltpu.VMEM((jobs, nz * rg, f), BF),
            dma((3, jobs)), dma((3,)), dma((3, 3)),
            [(dma, dma((n // 2, jobs))) for n in steps],
        ],
        compiler_params=pltpu.CompilerParams(vmem_limit_bytes=GATHER_VMEM, collective_id=1, has_side_effects=True),
        name="gather",
    )(sums, m, v, weights)


def emit_kernel(gathered, sums, m, v, outs, new_m, new_v, hold, sums_held, m_held, v_held, sems, small_sems):
    g, u, d = gathered
    go, uo, do = outs
    copies = [pltpu.make_async_copy(a.at[i], b.at[i], sems.at[k, i]) for k, (a, b) in enumerate(((g, go), (u, uo))) for i in range(2)]
    parts = [(i, x) for i in range(2) for x in range(d.shape[1])]
    slots = hold.shape[0]
    ins = [pltpu.make_async_copy(d.at[p], hold.at[k % slots], sems.at[2, k]) for k, p in enumerate(parts)]
    writes = [pltpu.make_async_copy(hold.at[k % slots], do.at[p], sems.at[3, k]) for k, p in enumerate(parts)]
    small = [pltpu.make_async_copy(a[k], b[k], small_sems.at[i, k]) for i, (a, b) in enumerate(((sums, sums_held), (m, m_held), (v, v_held))) for k in range(3)]
    back = [pltpu.make_async_copy(a[k], b[k], small_sems.at[3 + i, k]) for i, (a, b) in enumerate(((m_held, new_m), (v_held, new_v))) for k in range(3)]
    for c in small + ins[:slots] + copies:
        c.start()
    for c in small:
        c.wait()
    for k in range(3):
        _, m_held[k][ALL], v_held[k][ALL] = adamw(None, m_held[k][ALL], v_held[k][ALL], sums_held[k][ALL])
    for c in back:
        c.start()
    for k in range(len(parts)):
        ins[k].wait()
        writes[k].start()
        if k >= 1 and k - 1 + slots < len(parts):
            writes[k - 1].wait()
            ins[k - 1 + slots].start()
    for c in writes[len(parts) - slots:] + copies + back:
        c.wait()


def emit(gathered, sums, m, v):
    vmem, hbm = pl.BlockSpec(memory_space=pltpu.VMEM), pl.BlockSpec(memory_space=pltpu.HBM)
    dma = pltpu.SemaphoreType.DMA
    moments = [jax.ShapeDtypeStruct(a.shape, F32) for a in m]
    held = [pltpu.VMEM(a.shape, F32) for a in m]
    outs, new_m, new_v = pl.pallas_call(
        emit_kernel,
        in_specs=[[vmem, vmem, hbm], [hbm] * 3, [hbm] * 3, [hbm] * 3],
        out_specs=[[hbm] * 3, [hbm] * 3, [hbm] * 3],
        out_shape=[[jax.ShapeDtypeStruct(a.shape, BF) for a in gathered], moments, moments],
        scratch_shapes=[pltpu.VMEM((3, *gathered[2].shape[2:]), BF), held, held, held, dma((4, 8)), dma((5, 3))],
        compiler_params=pltpu.CompilerParams(vmem_limit_bytes=EMIT_VMEM),
        name="emit",
    )(gathered, sums, m, v)
    return (*(a.reshape(2, -1, w.shape[2]) for a, w in zip(outs, m, strict=True)), *new_m, *new_v)


def adamw(w, m, v, g):
    g = g.astype(BF).astype(F32)
    m = 0.9 * m + 0.1 * g
    v = 0.95 * v + 0.05 * g * g
    if w is None:
        return None, m, v
    step = m * lax.rsqrt(v + 1e-8) + 0.1 * w
    return (w - 0.02 * step).astype(BF), m, v


def device_step(x, dy, *arrays):
    weights, m, v = (list(arrays[i:i + 3]) for i in (0, 3, 6))
    sums = gradients(x[0], dy[0], *weights)
    sums, m, v = ([pltpu.with_memory_space_constraint(t, pltpu.HBM) for t in ts] for ts in (sums, m, v))
    return emit(list(gather(sums, m, v, weights)), sums, m, v)


def solution(mesh):
    x, w, m = P(("rep", "dp"), None, None), P(None, None, None), P(None, "dp", None)
    return jax.shard_map(
        device_step,
        mesh=mesh,
        in_specs=(x, x, w, w, w, *[m] * 6),
        out_specs=(*[P("rep", None, None)] * 3, *[P("rep", "dp", None)] * 6),
        check_vma=False,
    )
```

```python
import functools

import jax
import jax.numpy as jnp
from jax import lax
from jax.experimental import pallas as pl
from jax.experimental.pallas import tpu as pltpu
from jax.sharding import PartitionSpec as P

GRID = (4, 4, 8)
BF, F32 = jnp.bfloat16, jnp.float32
ALL = Ellipsis
MESH = pl.DeviceIdType.MESH
VMEM_LIMIT = 66_000_000
GATHER_LAG = 4
EMIT_VMEM = 10 << 20
GATHER_VMEM = 12 << 20
LAG = 2
SLOTS = 6
GROUPS = 3
JOBS = 4


def dot(a, b, dims=((1,), (0,))):
    return lax.dot_general(a, b, (dims, ((), ())), preferred_element_type=F32)


def normed(h):
    wide = h.astype(F32)
    scale = lax.rsqrt(jnp.mean(wide**2, -1, keepdims=True) + 1e-6)
    return (wide * scale).astype(BF)


def place():
    nx, ny, nz = GRID
    me = lax.axis_index("dp")
    at = (lax.div(me, ny * nz), lax.rem(lax.div(me, nz), ny), lax.rem(me, nz))

    def neighbour(axis, step):
        c = list(at)
        c[axis] = lax.rem(at[axis] + (step + GRID[axis]), GRID[axis])
        return (c[0] * ny + c[1]) * nz + c[2]

    return at, neighbour


def greet(neighbour, whole):
    steps = [(axis, step) for axis in range(3) for step in (range(1, GRID[axis]) if whole else (1, GRID[axis] - 1))]
    for axis, step in steps:
        pl.semaphore_signal(pltpu.get_barrier_semaphore(), inc=1, device_id={"dp": neighbour(axis, step)}, device_id_type=MESH)
    return len(steps)


class Sender:
    def __init__(self, axis, at, neighbour, send, recv):
        self.n, self.p = GRID[axis], at[axis]
        self.to = (neighbour(axis, 1), neighbour(axis, -1))
        self.send, self.recv = send, recv
        self.slots = bool(send.shape)

    def block(self, step):
        return lax.rem(self.p + (step + self.n), self.n)

    def copy(self, step, slot, d, src, dst):
        return pltpu.make_async_remote_copy(
            src_ref=src, dst_ref=dst, send_sem=self.send.at[step, slot] if self.slots else self.send, recv_sem=self.recv.at[step, slot],
            device_id={"dp": self.to[d]}, device_id_type=MESH,
        )

    def wait(self, step, slot, both):
        for sem in (self.recv, self.send) if self.slots else (self.recv,):
            pltpu.make_async_copy(both, both, sem.at[step, slot]).wait()


class Direct:
    def __init__(self, axis, at, neighbour, own, stage, recv, send_sem, recv_sem):
        n, p = GRID[axis], at[axis]
        self.own, self.mine = own, p
        self.copies = []
        for q in range(1, n):
            copy = pltpu.make_async_remote_copy(
                src_ref=stage.at[q - 1], dst_ref=recv.at[q - 1], send_sem=send_sem.at[q - 1], recv_sem=recv_sem.at[q - 1],
                device_id={"dp": neighbour(axis, q)}, device_id_type=MESH,
            )
            self.copies.append((lax.rem(p + q, n), stage.at[q - 1], recv.at[q - 1], copy))

    def start(self):
        for block, stage, _, copy in self.copies:
            stage[ALL] = self.own(block)[ALL].astype(BF)
            copy.start()

    def finish(self):
        done = self.own(self.mine)[ALL]
        for _, _, recv, copy in self.copies:
            copy.wait_recv()
            copy.wait_send()
            done = done + recv[ALL].astype(F32)
        return done


def compute(layer, blocks, a_all, at_all, dh, wg, wu, wd, hid, dgate, dup, da):
    tokens = dgate.shape[0]
    rows = tokens // blocks
    for b in range(blocks):
        s = pl.ds(b * rows, rows)
        a = a_all[layer, s]
        gate = dot(a, wg)
        up = dot(a, wu)
        ct = dot(dh[layer, s], wd, ((1,), (1,))).astype(BF).astype(F32)
        sig = jax.nn.sigmoid(gate)
        silu = gate * sig
        hid[s] = (silu * up).astype(BF)
        dup[s] = (ct * silu).astype(BF)
        dgate[s] = (ct * up * (sig + silu * (1.0 - sig))).astype(BF)

    if layer == 1:
        da[ALL] += dot(dgate[ALL], wg, ((1,), (1,))) + dot(dup[ALL], wu, ((1,), (1,)))

    at = at_all[layer]
    return dot(at, dgate[ALL]), dot(at, dup[ALL]), dot(hid[ALL], dh[layer], ((0,), (0,)))


def reduce_kernel(x_in, dy_in, wg, wu, wd, out_g, out_u, out_d, *scratch):
    (x, in_sem, hid, dgate, dup, da, dh, a_all, at_all, h1,
     own_g, own_u, own_d, acc_g2, acc_u2, acc_w3, acc_d2, acc_d3,
     rg, ru, rw, rd, sg, su, sw, sd, sems, direct, hold_g, hold_u, hold_d, hold_sem) = scratch
    nx, ny, nz = GRID
    chunks = nx * ny
    total = 2 * chunks
    f = hold_g.shape[2]
    at, neighbour = place()

    senders = {
        name: Sender(axis, at, neighbour, *sem)
        for (name, axis), sem in zip(
            (("g1", 0), ("g2", 1), ("u1", 1), ("u2", 0), ("w3", 2), ("d1", 2), ("d2", 1), ("d3", 0)), sems, strict=True
        )
    }

    def halves(array, ref):
        if array == "w3":
            return ref.at[0], ref.at[1]
        h = ref.shape[0] // 2
        return ref.at[pl.ds(0, h)], ref.at[pl.ds(h, h)]

    def first(array, slot, own, recv):
        s = senders[array]

        def start():
            for d, half in enumerate(halves(array, own(s.block(s.n // 2)))):
                s.copy(0, slot, d, half, recv[0].at[slot, d]).start()

        def middle(j):
            s.wait(j - 1, slot, recv[j - 1].at[slot])
            q = s.n // 2 - j
            for d in (0, 1):
                block = own(s.block(q if d == 0 else -q))
                into = halves(array, block)[d] if j == 1 else block
                into[ALL] = (into[ALL].astype(F32) + recv[j - 1][slot, d].astype(F32)).astype(BF)
                s.copy(j, slot, d, block, recv[j].at[slot, d]).start()

        def last():
            j = s.n // 2
            s.wait(j - 1, slot, recv[j - 1].at[slot])
            return own(s.p)[ALL].astype(F32) + recv[j - 1][slot, 0].astype(F32) + recv[j - 1][slot, 1].astype(F32)

        return start, middle, last

    def later(array, slot, own, recv, stage):
        s = senders[array]

        def start():
            for d, half in enumerate(halves(array, own(s.block(s.n // 2)))):
                stage[0][slot, d] = half[ALL].astype(BF)
                s.copy(0, slot, d, stage[0].at[slot, d], recv[0].at[slot, d]).start()

        def middle(j):
            s.wait(j - 1, slot, recv[j - 1].at[slot])
            q = s.n // 2 - j
            for d in (0, 1):
                block = own(s.block(q if d == 0 else -q))
                into = halves(array, block)[d] if j == 1 else block
                into[ALL] = into[ALL] + recv[j - 1][slot, d].astype(F32)
                stage[j][slot, d] = block[ALL].astype(BF)
                s.copy(j, slot, d, stage[j].at[slot, d], recv[j].at[slot, d]).start()

        def last():
            j = s.n // 2
            s.wait(j - 1, slot, recv[j - 1].at[slot])
            return own(s.p)[ALL] + recv[j - 1][slot, 0].astype(F32) + recv[j - 1][slot, 1].astype(F32)

        return start, middle, last

    def layer_of(c):
        return 1 - lax.div(c, chunks)

    def enter(layer, h):
        a = normed(h)
        a_all[layer] = a
        at_all[layer] = a.T

    loads = [pltpu.make_async_copy(a, b, in_sem.at[k]) for k, (a, b) in enumerate(((x_in, x), (dy_in, dh.at[1])))]

    def begin():
        loads[0].wait()
        enter(0, x[ALL])
        da[ALL] = jnp.zeros_like(da)

    def between():
        loads[1].wait()
        h = x[ALL] + da[ALL].astype(BF)
        h1[ALL] = h
        enter(1, h)
        da[ALL] = jnp.zeros_like(da)

    def weights(i, act):
        slot, layer = lax.rem(i, 2), lax.rem(lax.div(i, chunks), 2)
        part = pl.ds(pl.multiple_of(lax.rem(i, chunks) * f, f), f)
        for k, (src, dst) in enumerate(((wg.at[layer, :, part], hold_g), (wu.at[layer, :, part], hold_u), (wd.at[layer, part], hold_d))):
            act(pltpu.make_async_copy(src, dst.at[slot], hold_sem.at[slot, k]))

    def next_weights(i):
        weights(i, lambda c: c.wait())
        pl.when(i + 1 < 3 * chunks)(lambda: weights(i + 1, lambda c: c.start()))
        slot = lax.rem(i, 2)
        return hold_g[slot], hold_u[slot], hold_d[slot]

    def forward(i):
        g, u, d = next_weights(i)
        rows = hid.shape[0] // 2
        for b in range(2):
            s = pl.ds(b * rows, rows)
            gate = dot(a_all[0, s], g)
            up = dot(a_all[0, s], u)
            da[s] += dot((gate * jax.nn.sigmoid(gate) * up).astype(BF), d)

    def exchange(t):
        rings(t, lambda k, every, keep: stage(t, k, every, keep))

    def stage(t, k, every, keep):
        def run(fn):
            c = t - LAG * k
            on = (c >= 0) & (c < total)
            if every > 1:
                on &= lax.rem(c, every) == every - 1
            if keep is not None:
                on &= (c < total - 1) if keep == "early" else (c == total - 1)
            pl.when(on)(functools.partial(fn, c))

        return run

    def rings(t, at_point):
        def at_stage(k, every=1, keep=None):
            return at_point(k, every, keep)

        def d1(c):
            slot, long = lax.rem(c, SLOTS), lax.rem(c, 2 * SLOTS)
            return first("d1", slot, lambda q: own_d.at[long, q], rd[0:4])

        def d2(c):
            slot = lax.rem(lax.div(c, ny), 2)
            return later("d2", slot, lambda q: acc_d2.at[slot, q], rd[4:6], sd[0:2])

        def d3(c):
            slot = layer_of(c)
            return later("d3", slot, lambda q: acc_d3.at[slot, q], rd[6:8], sd[2:4])

        def d2_direct():
            slot = ((total - 1) // ny) % 2
            return Direct(1, at, neighbour, lambda q: acc_d2.at[slot, q], *direct[1])

        def d3_direct():
            return Direct(0, at, neighbour, lambda q: acc_d3.at[0, q], *direct[2])

        def d_last1(c):
            acc_d3[0, nx - 1] = d2_direct().finish()
            d3_direct().start()

        def d_last2(c):
            out_d[0] = d3_direct().finish()

        def d_end(c):
            out_d[layer_of(c)] = d3(c)[2]()

        def d_turn2(c):
            acc_d3[layer_of(c), lax.rem(lax.div(c, ny), nx)] = d2(c)[2]()

        def d_turn1(c):
            acc_d2[lax.rem(lax.div(c, ny), 2), lax.rem(c, ny)] = d1(c)[2]()

        at_stage(8, chunks, "early")(d_end)
        at_stage(7, chunks, "early")(lambda c: d3(c)[1](1))
        at_stage(6, ny, "early")(d_turn2)
        at_stage(6, chunks, "early")(lambda c: d3(c)[0]())
        at_stage(5, ny, "early")(lambda c: d2(c)[1](1))
        at_stage(6, ny, "last")(d_last2)
        at_stage(5, ny, "last")(d_last1)
        at_stage(4)(d_turn1)
        at_stage(4, ny, "early")(lambda c: d2(c)[0]())
        at_stage(4, ny, "last")(lambda c: d2_direct().start())
        for j in (3, 2, 1):
            at_stage(j)(lambda c, j=j: d1(c)[1](j))

        def w3(c):
            slot = lax.rem(lax.div(c, ny), GROUPS)
            return later("w3", slot, lambda q: acc_w3.at[slot, q], rw, sw)

        def w_direct():
            slot = ((total - 1) // ny) % GROUPS
            return Direct(2, at, neighbour, lambda q: acc_w3.at[slot, q], *direct[0])

        def w_end(c, last=False):
            done = w_direct().finish() if last else w3(c)[2]()
            cols = pl.ds(pl.multiple_of(lax.div(lax.rem(c, chunks), ny) * (ny * f), ny * f), ny * f)
            out_g[layer_of(c), :, cols] = done[0]
            out_u[layer_of(c), :, cols] = done[1]

        at_stage(8, ny, "early")(w_end)
        at_stage(5, ny, "last")(lambda c: w_end(c, True))
        for j in (3, 2, 1):
            at_stage(4 + j, ny, "early")(lambda c, j=j: w3(c)[1](j))

        def wide(which, own, acc2, recv, stage):
            def own1(slot):
                return (lambda q: own.at[slot, q]) if which == "g" else (lambda q: own.at[slot, :, q])

            def p1(c):
                slot = lax.rem(c, SLOTS)
                return first(which + "1", slot, own1(slot), recv[0:2])

            def p2(c):
                slot = lax.rem(c, SLOTS)
                return later(which + "2", slot, lambda q: acc2.at[slot, q], recv[2:4], stage[0:2])

            def turn2(c):
                done = p2(c)[2]()
                rows = acc_w3.shape[3]
                cols = pl.ds(pl.multiple_of(lax.rem(c, ny) * f, f), f)
                for q in range(nz):
                    acc_w3[lax.rem(lax.div(c, ny), GROUPS), q, "gu".index(which), :, cols] = done[q * rows:(q + 1) * rows]

            at_stage(4)(turn2)
            at_stage(3)(lambda c: p2(c)[1](1))

            def turn1(c):
                done = p1(c)[2]()
                acc2[lax.rem(c, SLOTS)] = done.reshape(acc2.shape[1:])
                p2(c)[0]()

            at_stage(2)(turn1)
            at_stage(1)(lambda c: p1(c)[1](1))

        wide("g", own_g, acc_g2, rg, sg)
        wide("u", own_u, acc_u2, ru, su)
        at_stage(4, ny, "early")(lambda c: w3(c)[0]())
        at_stage(4, ny, "last")(lambda c: w_direct().start())

    def backward_norm():
        h, by_a = h1[ALL].astype(F32), da[ALL].astype(BF).astype(F32)
        scale = lax.rsqrt(jnp.mean(h**2, -1, keepdims=True) + 1e-6)
        by_h = scale * by_a - h * (scale**3 * jnp.mean(by_a * h, -1, keepdims=True))
        dh[0] = dh[1] + by_h.astype(BF)

    def produce(layer, c):
        slot, long = lax.rem(c, SLOTS), lax.rem(c, 2 * SLOTS)
        g, u, d = compute(layer, 4, a_all, at_all, dh, *next_weights(chunks + c), hid, dgate, dup, da)
        own_g[slot] = g.astype(BF).reshape(own_g.shape[1:])
        own_u[slot] = u.astype(BF).reshape(own_u.shape[1:])
        own_d[long] = d.astype(BF).reshape(own_d.shape[1:])
        first("d1", slot, lambda q: own_d.at[long, q], rd[0:4])[0]()
        first("g1", slot, lambda q: own_g.at[slot, q], rg[0:2])[0]()
        first("u1", slot, lambda q: own_u.at[slot, :, q], ru[0:2])[0]()

    def ticks(start, stop, *fns):
        def tick(t, carry):
            for fn in fns:
                fn(t)
            return carry

        lax.fori_loop(start, stop, tick, 0)

    for c in loads:
        c.start()
    weights(0, lambda c: c.start())
    met = greet(neighbour, True)
    begin()
    ticks(0, chunks, forward)
    pl.semaphore_wait(pltpu.get_barrier_semaphore(), met)
    between()
    ticks(0, chunks, exchange, functools.partial(produce, 1))
    backward_norm()
    ticks(chunks, total, exchange, functools.partial(produce, 0))
    ticks(total, max(total - 1 + 6 * LAG, total - 1 - ny + 8 * LAG) + 1, exchange)


def gradients(x, dy, wg, wu, wd):
    nx, ny, nz = GRID
    n = nx * ny * nz
    tokens, d = x.shape
    ff = wg.shape[2]
    chunks = nx * ny
    f, rg, rd = ff // chunks, d // n, ff // n
    total = 2 * chunks

    s, long = SLOTS, 2 * SLOTS
    g_blocks = [((ny * nz * rg) // 2, f), (ny * nz * rg, f), (nz * rg // 2, f), (nz * rg, f)]
    u_blocks = [(nx // 2, nz * rg, f), (nx, nz * rg, f), (nz * rg // 2, f), (nz * rg, f)]
    w_blocks = [(rg, ny * f)] + [(2, rg, ny * f)] * (nz // 2 - 1)
    d_blocks = [(rd // 2, d)] + [(rd, d)] * (nz // 2 - 1) + [(rd // 2, d), (rd, d)] * 2
    d_slots = [s] * (nz // 2) + [2] * 4
    steps = {"g1": nx, "g2": ny, "u1": ny, "u2": nx, "w3": nz, "d1": nz, "d2": ny, "d3": nx}
    dma = pltpu.SemaphoreType.DMA

    def sems(name, n):
        count = {"d2": 2, "d3": 2, "w3": GROUPS}.get(name, s)
        return (dma((n // 2, count)), dma((n // 2, count)))

    scratch = [
        pltpu.VMEM((tokens, d), BF), dma((2,)),
        pltpu.VMEM((tokens, f), BF), pltpu.VMEM((tokens, f), BF), pltpu.VMEM((tokens, f), BF),
        pltpu.VMEM((tokens, d), F32), pltpu.VMEM((2, tokens, d), BF),
        pltpu.VMEM((2, tokens, d), BF), pltpu.VMEM((2, d, tokens), BF), pltpu.VMEM((tokens, d), BF),
        pltpu.VMEM((s, nx, ny * nz * rg, f), BF), pltpu.VMEM((s, nx, ny, nz * rg, f), BF), pltpu.VMEM((long, nz, rd, d), BF),
        pltpu.VMEM((s, ny, nz * rg, f), F32), pltpu.VMEM((s, nx, nz * rg, f), F32),
        pltpu.VMEM((GROUPS, nz, 2, rg, ny * f), F32),
        pltpu.VMEM((2, ny, rd, d), F32), pltpu.VMEM((2, nx, rd, d), F32),
        [pltpu.VMEM((s, 2, *b), BF) for b in g_blocks],
        [pltpu.VMEM((s, 2, *b), BF) for b in u_blocks],
        [pltpu.VMEM((GROUPS, 2, *b), BF) for b in w_blocks],
        [pltpu.VMEM((k, 2, *b), BF) for k, b in zip(d_slots, d_blocks, strict=True)],
        [pltpu.VMEM((s, 2, *b), BF) for b in g_blocks[2:]],
        [pltpu.VMEM((s, 2, *b), BF) for b in u_blocks[2:]],
        [pltpu.VMEM((GROUPS, 2, *b), BF) for b in w_blocks],
        [pltpu.VMEM((k, 2, *b), BF) for k, b in zip(d_slots[nz // 2:], d_blocks[nz // 2:], strict=True)],
        [sems(name, n) for name, n in steps.items()],
        [
            (pltpu.VMEM((n - 1, *b), BF), pltpu.VMEM((n - 1, *b), BF), dma((n - 1,)), dma((n - 1,)))
            for n, b in ((nz, (2, rg, ny * f)), (ny, (rd, d)), (nx, (rd, d)))
        ],
        pltpu.VMEM((2, d, f), BF), pltpu.VMEM((2, d, f), BF), pltpu.VMEM((2, f, d), BF), dma((2, 3)),
    ]
    vmem = pl.BlockSpec(memory_space=pltpu.VMEM)
    return pl.pallas_call(
        reduce_kernel,
        in_specs=[pl.BlockSpec(memory_space=pl.ANY)] * 5,
        out_specs=[vmem] * 3,
        out_shape=[jax.ShapeDtypeStruct((2, rg, ff), F32)] * 2 + [jax.ShapeDtypeStruct((2, rd, d), F32)],
        scratch_shapes=scratch,
        compiler_params=pltpu.CompilerParams(
            vmem_limit_bytes=VMEM_LIMIT, collective_id=0, has_side_effects=True
        ),
        name="reduce",
    )(x, dy, wg, wu, wd)


def gather_kernel(sums, m, v, weights, og, ou, od, *scratch):
    ng, nu, nd, rows_gu, rows_d, sums_held, m_held, v_held, zb, yg, yu, local, rows_sem, held_sem, sems = scratch
    nx, ny, nz = GRID
    total = 2 * JOBS
    f, r = zb.shape[-1], nd.shape[1] // JOBS
    at, neighbour = place()
    x_, y_, z_ = at
    met = greet(neighbour, False)
    me = lax.axis_index("dp")
    rg, rd = ng.shape[1], nd.shape[1]
    eight = pl.ds(pl.multiple_of(lax.div(me, 8 // rg) * 8, 8), 8)
    own = [pltpu.make_async_copy(w.at[:, eight], rows_gu.at[k], rows_sem.at[k]) for k, w in enumerate(weights[:2])]
    own.append(pltpu.make_async_copy(weights[2].at[:, pl.ds(pl.multiple_of(me * rd, rd), rd)], rows_d, rows_sem.at[2]))
    for i, (a, b) in enumerate(((sums, sums_held), (m, m_held), (v, v_held))):
        own += [pltpu.make_async_copy(a[k], b[k], held_sem.at[i, k]) for k in range(3)]
    for c in own:
        c.start()
    for c in own:
        c.wait()
    upper = lax.rem(me, 8 // rg) == 1
    for k, new in enumerate((ng, nu)):
        w = jnp.where(upper, rows_gu[k, :, rg:].astype(F32), rows_gu[k, :, :rg].astype(F32))
        new[ALL] = adamw(w, m_held[k][ALL], v_held[k][ALL], sums_held[k][ALL])[0]
    nd[ALL] = adamw(rows_d[ALL].astype(F32), m_held[2][ALL], v_held[2][ALL], sums_held[2][ALL])[0]
    names = (("w1", 2), ("g2", 1), ("g3", 0), ("u2", 0), ("u3", 1), ("d1", 0), ("d2", 1), ("d3", 2))
    odd = (("e1", 1), ("e2", 0), ("e3", 2))
    senders = {name: Sender(axis, at, neighbour, *sem) for (name, axis), sem in zip((*names, *odd), (*sems, *sems[5:]), strict=True)}

    def piece(j):
        return 1 - lax.div(j, JOBS), lax.rem(j, JOBS)

    def blocks(name, j):
        layer, q = piece(j)
        cols, rows = pl.ds(pl.multiple_of(q * f, f), f), pl.ds(pl.multiple_of(q * r, r), r)
        h = nz * ng.shape[1] // 2
        d = nd.shape[2] // 2

        def halves(at_half, n):
            return lambda b: tuple(at_half(b, part) for part in (pl.ds(0, n), pl.ds(n, n)))

        return {
            "w1": (lambda b: zb.at[j, b], lambda b: (zb.at[j, b, 0], zb.at[j, b, 1])),
            "g2": (lambda b: og.at[layer, x_, b, :, cols], halves(lambda b, p: og.at[layer, x_, b, p, cols], h)),
            "u2": (lambda b: ou.at[layer, b, y_, :, cols], halves(lambda b, p: ou.at[layer, b, y_, p, cols], h)),
            "g3": (lambda b: og.at[layer, b, :, :, cols], halves(lambda b, p: og.at[layer, b, p, :, cols], ny // 2)),
            "u3": (lambda b: ou.at[layer, :, b, :, cols], halves(lambda b, p: ou.at[layer, p, b, :, cols], nx // 2)),
            "d1": (lambda b: od.at[layer, b, y_, z_, rows], halves(lambda b, p: od.at[layer, b, y_, z_, rows, p], d)),
            "e1": (lambda b: od.at[layer, x_, b, z_, rows], halves(lambda b, p: od.at[layer, x_, b, z_, rows, p], d)),
            "d2": (lambda b: od.at[layer, :, b, z_, rows], halves(lambda b, p: od.at[layer, p, b, z_, rows], nx // 2)),
            "e2": (lambda b: od.at[layer, b, :, z_, rows], halves(lambda b, p: od.at[layer, b, p, z_, rows], ny // 2)),
            "d3": (lambda b: od.at[layer, :, :, b, rows], halves(lambda b, p: od.at[layer, p, :, b, rows], nx // 2)),
            "e3": (lambda b: od.at[layer, :, :, b, rows], halves(lambda b, p: od.at[layer, p, :, b, rows], nx // 2)),
        }[name]

    def ring(name, j, i, first=None):
        s = senders[name]
        full, half = blocks(name, j)
        if i > 0:
            arrived(name, j, i - 1)
        for d in (0, 1):
            b = s.block(-i if d == 0 else i)
            dst = full(b) if i < s.n // 2 - 1 else half(b)[d]
            s.copy(i, j, d, first if first is not None else dst, dst).start()

    def arrived(name, j, i):
        s = senders[name]
        full = blocks(name, j)[0]
        s.wait(i, j, full(pl.ds(0, 2) if i < s.n // 2 - 1 else 0))

    def tick(t, carry):
        def at_stage(k, fn):
            j = t - GATHER_LAG * k
            pl.when((j >= 0) & (j < total))(lambda: fn(j))

        def keep(which, j):
            slot = j
            src, name, b = ((yg, "g2", y_), (yu, "u2", x_))[which]
            return pltpu.make_async_copy(src.at[slot], blocks(name, j)[0](b), local.at[which, slot])

        def begin(j):
            layer, q = piece(j)
            for k, new in enumerate((ng, nu)):
                zb[j, z_, k] = new[layer, :, pl.ds(pl.multiple_of(q * f, f), f)]
            ring("w1", j, 0)

        def turn(j):
            slot = j
            arrived("w1", j, nz // 2 - 1)
            for which, (yb, name) in enumerate(((yg, "g2"), (yu, "u2"))):
                yb[slot] = zb[j, :, which].reshape(yb.shape[1:])
                keep(which, j).start()
                ring(name, j, 0, yb.at[slot])

        def turn2(j):
            for which, name in enumerate("gu"):
                arrived(name + "2", j, 1)
                keep(which, j).wait()
                ring(name + "3", j, 0)

        def both(fn):
            def run(j):
                for name in "gu":
                    fn(name, j)

            return run

        k = nz // 2
        at_stage(k + 4, both(lambda name, j: arrived(name + "3", j, 1)))
        at_stage(k + 3, both(lambda name, j: ring(name + "3", j, 1)))
        at_stage(k + 2, turn2)
        at_stage(k + 1, both(lambda name, j: ring(name + "2", j, 1)))
        at_stage(k, turn)
        for i in range(k - 1, 0, -1):
            at_stage(i, lambda j, i=i: ring("w1", j, i))
        at_stage(0, begin)

        def own_rows(name, j):
            layer, q = piece(j)
            own = nd.at[layer, pl.ds(pl.multiple_of(q * r, r), r)]
            return own, pltpu.make_async_copy(own, blocks(name + "1", j)[0](x_ if name == "d" else y_), local.at[2, j])

        def d_begin(name, j):
            own, copy = own_rows(name, j)
            copy.start()
            ring(name + "1", j, 0, own)

        def d_turn(name, j):
            arrived(name + "1", j, 1)
            own_rows(name, j)[1].wait()
            ring(name + "2", j, 0)

        def d_turn2(name, j):
            arrived(name + "2", j, 1)
            ring(name + "3", j, 0)

        def either(k, fn):
            at_stage(k, lambda j: pl.when(lax.rem(j, 2) == 0)(lambda: fn("d", j)))
            at_stage(k, lambda j: pl.when(lax.rem(j, 2) == 1)(lambda: fn("e", j)))

        either(4 + k, lambda name, j: arrived(name + "3", j, k - 1))
        for i in range(k - 1, 0, -1):
            either(4 + i, lambda name, j, i=i: ring(name + "3", j, i))
        either(4, d_turn2)
        either(3, lambda name, j: ring(name + "2", j, 1))
        either(2, d_turn)
        either(1, lambda name, j: ring(name + "1", j, 1))
        either(0, d_begin)
        return carry

    pl.semaphore_wait(pltpu.get_barrier_semaphore(), met)
    lax.fori_loop(0, total + GATHER_LAG * (nz // 2 + 4), tick, 0)
    xs, ys, zs = (pl.ds(0, n - 1) for n in GRID)
    sent = (zb.at[:, zs], og.at[:, xs, 0], og.at[:, xs], ou.at[:, ys, 0], ou.at[:, :, ys], od.at[:, xs, 0, 0], od.at[:, :, ys, 0], od.at[:, :, :, zs])
    for (send, _), what in zip(sems, sent, strict=True):
        pltpu.make_async_copy(what, what, send).wait()


def gather(sums, m, v, weights):
    nx, ny, nz = GRID
    _, rg, ff = sums[0].shape
    _, rd, d = sums[2].shape
    hbm = [pl.BlockSpec(memory_space=pltpu.HBM)] * 3
    held = [pltpu.VMEM(a.shape, F32) for a in m]
    f, jobs = ff // JOBS, 2 * JOBS
    dma = pltpu.SemaphoreType.DMA
    steps = (nz, ny, nx, nx, ny, nx, ny, nz)
    wide = jax.ShapeDtypeStruct((2, nx, ny, nz * rg, ff), BF)
    return pl.pallas_call(
        gather_kernel,
        in_specs=[hbm] * 4,
        out_specs=[pl.BlockSpec(memory_space=pl.ANY)] * 3,
        out_shape=[wide, wide, jax.ShapeDtypeStruct((2, nx, ny, nz, rd, d), BF)],
        scratch_shapes=[
            pltpu.VMEM((2, rg, ff), BF), pltpu.VMEM((2, rg, ff), BF), pltpu.VMEM((2, rd, d), BF),
            pltpu.VMEM((2, 2, 8, ff), BF), pltpu.VMEM((2, rd, d), BF), held, held, held,
            pltpu.VMEM((jobs, nz, 2, rg, f), BF), pltpu.VMEM((jobs, nz * rg, f), BF), pltpu.VMEM((jobs, nz * rg, f), BF),
            dma((3, jobs)), dma((3,)), dma((3, 3)),
            [(dma, dma((n // 2, jobs))) for n in steps],
        ],
        compiler_params=pltpu.CompilerParams(vmem_limit_bytes=GATHER_VMEM, collective_id=1, has_side_effects=True),
        name="gather",
    )(sums, m, v, weights)


def emit_kernel(gathered, sums, m, v, outs, new_m, new_v, hold, sums_held, m_held, v_held, sems, small_sems):
    g, u, d = gathered
    go, uo, do = outs
    copies = [pltpu.make_async_copy(a.at[i], b.at[i], sems.at[k, i]) for k, (a, b) in enumerate(((g, go), (u, uo))) for i in range(2)]
    parts = [(i, x) for i in range(2) for x in range(d.shape[1])]
    slots = hold.shape[0]
    ins = [pltpu.make_async_copy(d.at[p], hold.at[k % slots], sems.at[2, k]) for k, p in enumerate(parts)]
    writes = [pltpu.make_async_copy(hold.at[k % slots], do.at[p], sems.at[3, k]) for k, p in enumerate(parts)]
    small = [pltpu.make_async_copy(a[k], b[k], small_sems.at[i, k]) for i, (a, b) in enumerate(((sums, sums_held), (m, m_held), (v, v_held))) for k in range(3)]
    back = [pltpu.make_async_copy(a[k], b[k], small_sems.at[3 + i, k]) for i, (a, b) in enumerate(((m_held, new_m), (v_held, new_v))) for k in range(3)]
    for c in ins[:slots] + copies + small:
        c.start()
    for k in range(len(parts)):
        if k == slots:
            for c in small:
                c.wait()
            for mk, vk, sk in zip(m_held, v_held, sums_held, strict=True):
                _, mk[ALL], vk[ALL] = adamw(None, mk[ALL], vk[ALL], sk[ALL])
        ins[k].wait()
        writes[k].start()
        if k >= 1 and k - 1 + slots < len(parts):
            writes[k - 1].wait()
            ins[k - 1 + slots].start()
        if k == slots:
            for c in back:
                c.start()
    for c in writes[len(parts) - slots:] + copies + back:
        c.wait()


def emit(gathered, sums, m, v):
    vmem, hbm = pl.BlockSpec(memory_space=pltpu.VMEM), pl.BlockSpec(memory_space=pltpu.HBM)
    dma = pltpu.SemaphoreType.DMA
    moments = [jax.ShapeDtypeStruct(a.shape, F32) for a in m]
    held = [pltpu.VMEM(a.shape, F32) for a in m]
    outs, new_m, new_v = pl.pallas_call(
        emit_kernel,
        in_specs=[[vmem, vmem, hbm], [hbm] * 3, [hbm] * 3, [hbm] * 3],
        out_specs=[[hbm] * 3, [hbm] * 3, [hbm] * 3],
        out_shape=[[jax.ShapeDtypeStruct(a.shape, BF) for a in gathered], moments, moments],
        scratch_shapes=[pltpu.VMEM((3, *gathered[2].shape[2:]), BF), held, held, held, dma((4, 8)), dma((5, 3))],
        compiler_params=pltpu.CompilerParams(vmem_limit_bytes=EMIT_VMEM),
        name="emit",
    )(gathered, sums, m, v)
    return (*(a.reshape(2, -1, w.shape[2]) for a, w in zip(outs, m, strict=True)), *new_m, *new_v)


def adamw(w, m, v, g):
    g = g.astype(BF).astype(F32)
    m = 0.9 * m + 0.1 * g
    v = 0.95 * v + 0.05 * g * g
    if w is None:
        return None, m, v
    step = m * lax.rsqrt(v + 1e-8) + 0.1 * w
    return (w - 0.02 * step).astype(BF), m, v


def device_step(x, dy, *arrays):
    weights, m, v = (list(arrays[i:i + 3]) for i in (0, 3, 6))
    sums = gradients(x[0], dy[0], *weights)
    sums, m, v = ([pltpu.with_memory_space_constraint(t, pltpu.HBM) for t in ts] for ts in (sums, m, v))
    return emit(list(gather(sums, m, v, weights)), sums, m, v)


def solution(mesh):
    x, w, m = P(("rep", "dp"), None, None), P(None, None, None), P(None, "dp", None)
    return jax.shard_map(
        device_step,
        mesh=mesh,
        in_specs=(x, x, w, w, w, *[m] * 6),
        out_specs=(*[P("rep", None, None)] * 3, *[P("rep", "dp", None)] * 6),
        check_vma=False,
    )
```
